32 devices in a mesh: lat: 4 (over x, core), lon: 8 (over z, y).
Axes of the slice: x: 2, y: 2, z: 4, core: 2. Of those that a mesh axis runs over, the one named last changes fastest.
Arguments:
- tokens: bfloat16 [4, 48, 96, 512], P(None, 'lat', 'lon'), may hold values from -6 to 6
- region: int32 [4, 48, 96], P(None, 'lat', 'lon'), may hold values from 0 to 2
- norm_gain1: float32 [2, 512], replicated, may hold values from 0.25 to 1.75
- qkv_weight: bfloat16 [2, 512, 1536], replicated, may hold values from -3 to 3
- proj_weight: bfloat16 [2, 512, 512], replicated, may hold values from -0.25 to 0.25
- norm_gain2: float32 [2, 512], replicated, may hold values from 0.25 to 1.75
- up_weight: bfloat16 [2, 512, 2048], replicated, may hold values from -0.25 to 0.25
- down_weight: bfloat16 [2, 2048, 512], replicated, may hold values from -0.125 to 0.125
Outputs:
- result: bfloat16 [4, 48, 96, 512], P(None, 'lat', 'lon')
The draws below stay inside these ranges and needn't reach their ends.
All inputs are finite; a program needn't handle non-finite values.
Results may differ from the reference program's by a relative error of at most 0.012.
Values may be sent and summed in bfloat16 or wider, within the bound.
A program may use at most 64 MiB of HBM per device.

```python
import math
import jax
import jax.numpy as jnp
from jax import lax

D = 512
FF = 2048
HEADS = 8
LEV = 4
WLEV = 2
WLAT = 6
WLON = 12
NLAT = 48
NLON = 96


def draw_qkv_weight(key, part):
    first_key = jax.random.fold_in(jax.random.fold_in(key, 17), 0)
    base = jax.random.normal(first_key, (2, D, 3 * D), jnp.float32) / math.sqrt(D)
    return base.astype(jnp.bfloat16)


def plant(values, key, least, largest):
    longest = values.shape.index(max(values.shape))
    spots = []
    for shift in (0, 1):
        where = [jax.random.randint(jax.random.fold_in(key, axis), (), 0, length) for axis, length in enumerate(values.shape)]
        where[longest] = (where[longest] + shift) % values.shape[longest]
        spots.append(tuple(where))
    return values.at[spots[0]].set(least).at[spots[1]].set(largest)


def block_levels(rng, shape, cuts, low, largest):
    factor_of, own = 1.0, jax.random.fold_in(rng, 6)
    for axis_at, parts in cuts:
        steps = jnp.exp(jax.random.uniform(jax.random.fold_in(own, axis_at), (parts,), jnp.float32, low / len(cuts), largest / len(cuts)))
        factor_of = factor_of * jnp.repeat(steps, shape[axis_at] // parts).reshape([-1 if axis == axis_at else 1 for axis in range(len(shape))])
    return factor_of


def bell_draw(key, extent, scale, limit, cuts=(), held_as=jnp.bfloat16):
    drawn = jax.random.normal(key, extent, jnp.float32) * scale
    if len(cuts) > 0:
        drawn = block_levels(key, extent, cuts, -0.22, 0.18) * drawn
    return jnp.clip(drawn, min=-limit, max=limit).astype(held_as)


def setup_inputs(seed: int = 0) -> dict:
    splits = jax.random.split(jax.random.key(seed), 9)
    tokens = bell_draw(splits[0], (LEV, NLAT, NLON, D), 1.0, 6.0, ((1, 4), (2, 8)))
    region = plant(jax.random.randint(splits[1], (LEV, NLAT, NLON), 0, 3), jax.random.fold_in(splits[1], 1), 0, 2).astype(jnp.int32)
    norm_gain1 = jnp.clip(1.0 + 0.15 * jax.random.normal(splits[2], (2, D), jnp.float32), 0.25, 1.75)
    qkv_weight = draw_qkv_weight(jax.random.fold_in(splits[8], 71), 0)
    proj_weight = bell_draw(splits[4], (2, D, D), D ** -0.5, 0.25)
    norm_gain2 = jnp.clip(1.0 + 0.15 * jax.random.normal(splits[5], (2, D), jnp.float32), 0.25, 1.75)
    up_weight = bell_draw(splits[6], (2, D, FF), D ** -0.5, 0.25)
    down_weight = bell_draw(splits[7], (2, FF, D), FF ** -0.5, 0.125)
    return {"tokens": tokens, "region": region, "norm_gain1": norm_gain1, "qkv_weight": qkv_weight, "proj_weight": proj_weight, "norm_gain2": norm_gain2, "up_weight": up_weight, "down_weight": down_weight}


epsilon = 1e-05

def layer_norm(field, gain_vector):
    field = field.astype(jnp.float32)
    average = lax.optimization_barrier(jnp.mean(field, axis=-1, keepdims=True))
    centered = field - average
    variance = lax.optimization_barrier(jnp.mean(centered * centered, axis=-1, keepdims=True))
    return centered * lax.rsqrt(variance + epsilon) * gain_vector

def to_windows(field):
    level_count, row_count, column_count = field.shape[:3]
    trailing = tuple(field.shape[3:])
    shaped = field.reshape((level_count // WLEV, WLEV, row_count // WLAT, WLAT, column_count // WLON, WLON) + trailing)
    order = (0, 2, 4, 1, 3, 5) + tuple(range(6, 6 + len(trailing)))
    return jnp.transpose(shaped, order).reshape((-1, WLEV * WLAT * WLON) + trailing)

def from_windows(windows, level_count, row_count, column_count):
    trailing = tuple(windows.shape[2:])
    shaped = windows.reshape((level_count // WLEV, row_count // WLAT, column_count // WLON, WLEV, WLAT, WLON) + trailing)
    order = (0, 3, 1, 4, 2, 5) + tuple(range(6, 6 + len(trailing)))
    return jnp.transpose(shaped, order).reshape((level_count, row_count, column_count) + trailing)

def window_attention(normed, labels, w_qkv, w_proj):
    count, span, features = normed.shape
    head_size = features // HEADS
    mixed = jnp.dot(normed, w_qkv, preferred_element_type=jnp.float32).astype(jnp.bfloat16)
    queries = mixed[..., :features].reshape(count, span, HEADS, head_size).astype(jnp.float32)
    key_vectors = mixed[..., features:2 * features].reshape(count, span, HEADS, head_size).astype(jnp.float32)
    values = mixed[..., 2 * features:].reshape(count, span, HEADS, head_size).astype(jnp.float32)
    scores = jnp.einsum('wqhd,wkhd->whqk', queries, key_vectors) * (1.0 / math.sqrt(head_size))
    allowed = labels[:, None, :, None] == labels[:, None, None, :]
    scores = jnp.where(allowed, scores, -jnp.inf)
    peak = lax.optimization_barrier(jnp.max(scores, axis=-1, keepdims=True))
    exponent = jnp.exp(scores - peak)
    attention_weights = (exponent / lax.optimization_barrier(jnp.sum(exponent, axis=-1, keepdims=True))).astype(jnp.bfloat16)
    gathered = jnp.einsum('whqk,wkhd->wqhd', attention_weights.astype(jnp.float32), values)
    gathered = gathered.astype(jnp.bfloat16).reshape(count, span, features)
    return jnp.dot(gathered, w_proj, preferred_element_type=jnp.float32)

def attention_part(field, labels, gain_vector, w_qkv, w_proj):
    level_count, row_count, column_count, features = field.shape
    normed = layer_norm(field, gain_vector).astype(jnp.bfloat16)
    windows = to_windows(normed)
    window_labels = to_windows(labels)
    per_row = column_count // WLON
    groups = windows.reshape((-1, per_row) + tuple(windows.shape[1:]))
    label_groups = window_labels.reshape((-1, per_row) + tuple(window_labels.shape[1:]))

    def attend(pair):
        return window_attention(pair[0], pair[1], w_qkv, w_proj)
    projected = lax.map(attend, (groups, label_groups)).reshape(windows.shape)
    return field.astype(jnp.float32) + from_windows(projected, level_count, row_count, column_count)

def feed_forward(field, gain_vector, w_up, w_down):

    def per_level(level_field):
        normed = layer_norm(level_field, gain_vector).astype(jnp.bfloat16)
        hidden_units = jax.nn.gelu(jnp.dot(normed, w_up, preferred_element_type=jnp.float32)).astype(jnp.bfloat16)
        return (level_field + jnp.dot(hidden_units, w_down, preferred_element_type=jnp.float32)).astype(jnp.bfloat16)
    return lax.map(per_level, field)

def reference(tokens, region, norm_gain1, qkv_weight, proj_weight, norm_gain2, up_weight, down_weight):
    half_level = WLEV // 2
    half_row = WLAT // 2
    half_column = WLON // 2
    mixed_first = attention_part(tokens, region, norm_gain1[0], qkv_weight[0], proj_weight[0])
    first_out = feed_forward(mixed_first, norm_gain2[0], up_weight[0], down_weight[0])
    rolled = jnp.roll(first_out, (-half_level, -half_row, -half_column), (0, 1, 2))
    rolled_region = jnp.roll(region, (-half_level, -half_row, -half_column), (0, 1, 2))
    level_index = jnp.arange(LEV, dtype=jnp.int32)[:, None, None]
    row_index = jnp.arange(NLAT, dtype=jnp.int32)[None, :, None]
    wrapped_level = (level_index >= LEV - half_level).astype(jnp.int32)
    wrapped_row = (row_index >= NLAT - half_row).astype(jnp.int32)
    labels_second = rolled_region * 4 + wrapped_level * 2 + wrapped_row
    mixed_second = attention_part(rolled, labels_second, norm_gain1[1], qkv_weight[1], proj_weight[1])
    restored = jnp.roll(mixed_second, (half_level, half_row, half_column), (0, 1, 2))
    return feed_forward(restored, norm_gain2[1], up_weight[1], down_weight[1])
```

```python
import functools

import jax
import jax.numpy as jnp
from jax import lax
from jax.experimental import pallas as pl
from jax.experimental.pallas import tpu as pltpu
from jax.sharding import PartitionSpec as P

HEADS = 8
WLEV = 2
WLAT = 6
WLON = 12
EPSILON = 1e-05
FAR = -1e30
MESH = pl.DeviceIdType.MESH
F32 = jnp.float32
BF16 = jnp.bfloat16


def normed(field, gain):
    mean = jnp.mean(field, axis=-1, keepdims=True)
    centered = field - mean
    variance = jnp.mean(centered * centered, axis=-1, keepdims=True)
    return (centered * lax.rsqrt(variance + EPSILON) * gain).astype(BF16)


def gelu(x):
    inner = x * (0.7978845608028654 + 0.035677408136300125 * (x * x))
    half = 0.5 * x
    return half + half * jnp.tanh(inner)


def dot(a, b):
    return jnp.dot(a, b, preferred_element_type=F32)


def dot_t(a, b):
    return lax.dot_general(a, b, (((1,), (1,)), ((), ())), preferred_element_type=F32)


def kernel(
    x_ref, e_ref, g1_ref, g2_ref, wqkv_hbm, wproj_hbm, wup_hbm, wdown_hbm, out_ref,
    own, shift, back, eshift, xs, qkv, heads, marks_q, marks_k, inner,
    wqkv, wproj, wup, wdown, wsem, fsend, frecv, bsend, brecv, esend, erecv,
):
    lat_count, lon_count = lax.axis_size("lat"), lax.axis_size("lon")
    lat, lon = lax.axis_index("lat"), lax.axis_index("lon")
    up = lax.rem(lat + lat_count - 1, lat_count)
    down = lax.rem(lat + 1, lat_count)
    left = lax.rem(lon + lon_count - 1, lon_count)
    right = lax.rem(lon + 1, lon_count)
    before = {"left": (lat, left), "up": (up, lon), "corner": (up, left)}
    after = {"left": (lat, right), "up": (down, lon), "corner": (down, right)}

    weights = [
        pltpu.make_async_copy(source.at[block], target.at[block], wsem.at[block * 4 + at])
        for block in range(2)
        for at, (source, target) in enumerate(
            ((wqkv_hbm, wqkv), (wproj_hbm, wproj), (wup_hbm, wup), (wdown_hbm, wdown))
        )
    ]
    weights[0].start()
    weights[1].start()

    barrier = pltpu.get_barrier_semaphore()
    for device in list(before.values()) + list(after.values()):
        pl.semaphore_signal(barrier, inc=1, device_id=device, device_id_type=MESH)

    moves = (
        (2, 0, 0, "left"),
        (0, 1, 1, "corner"),
        (4, 0, 1, "left"),
        (6, 1, 0, "left"),
        (1, 1, 2, "up"),
    )
    local = {(0, 2): 3, (0, 3): 5, (1, 3): 7}
    arrivals = {(move[1], move[2]): at for at, move in enumerate(moves)}

    def label_copy(at):
        atom, window, place, towards = moves[at]
        return pltpu.make_async_remote_copy(
            e_ref.at[atom], eshift.at[window, place], esend.at[at], erecv.at[at],
            device_id=before[towards], device_id_type=MESH,
        )

    def forward_copy(at):
        atom, window, place, towards = moves[at]
        return pltpu.make_async_remote_copy(
            own.at[atom], shift.at[window, place], fsend.at[at], frecv.at[at],
            device_id=before[towards], device_id_type=MESH,
        )

    def backward_copy(at):
        atom, window, place, towards = moves[at]
        return pltpu.make_async_remote_copy(
            back.at[window, place], out_ref.at[atom], bsend.at[at], brecv.at[at],
            device_id=after[towards], device_id_type=MESH,
        )

    span, features = xs.shape[1:]
    half_span = span // 2
    size = span // 4
    piece = span // 8
    level_size = span // 16
    pair = 128
    hidden = wup.shape[2]
    step = 256
    lane = lax.broadcasted_iota(jnp.int32, (1, pair), 1)
    low = lane < 64
    scale = 64 ** -0.5
    head_masks = (
        jnp.where(low, scale, 0.0).astype(BF16),
        jnp.where(low, 0.0, scale).astype(BF16),
    )

    def to_pairs(block, pieces):
        pieces = [value.astype(F32) for value in pieces]
        if block == 0:
            order = [value[:piece] for value in pieces] + [value[piece:] for value in pieces]
        else:
            order = [value[level_size : level_size + piece] for value in pieces]
            for value in pieces:
                order += [value[level_size + piece :], value[:level_size]]
        return jnp.concatenate(order, axis=0)

    def from_pairs(block, first, second):
        if block == 0:
            order = [first, second]
        else:
            order = [second[level_size:], first, second[:level_size]]
        return jnp.concatenate(order, axis=0).astype(BF16)

    def prepare(block, at, pieces, marks_in):
        index = 2 * block + at
        marks = to_pairs(block, marks_in)
        half = low if block == 0 else jnp.logical_not(low)
        marks_q[index] = (marks * jnp.where(half, FAR, 0.0)).astype(BF16)
        marks_k[index] = (1.0 - marks).astype(BF16)
        x = to_pairs(block, pieces)
        xs[index] = x
        n1 = normed(x, g1_ref[block : block + 1, :])
        if at == 0:
            weights[block * 4].wait()
        qkv[index] = dot(n1, wqkv[block]).astype(BF16)

    def attend(block, at):
        index = 2 * block + at
        ones = jnp.ones((half_span, pair), BF16)
        for rows in (slice(0, half_span), slice(half_span, span)):
            mark_q = marks_q[index, rows, :]
            mark_q = jnp.concatenate([mark_q, mark_q], axis=0)
            mark_k = marks_k[index, rows, :]
            for column in range(0, features, pair):
                query = qkv[index, rows, column : column + pair]
                key = qkv[index, rows, features + column : features + column + pair]
                value = qkv[index, rows, 2 * features + column : 2 * features + column + pair]
                value = jnp.concatenate([value, ones], axis=1)
                query = jnp.concatenate([query * head_masks[0], query * head_masks[1]], axis=0)
                scores = dot_t(
                    jnp.concatenate([query, mark_q], axis=1),
                    jnp.concatenate([key, mark_k], axis=1),
                )
                peak = jnp.max(scores, axis=-1, keepdims=True)
                weight = jnp.exp(scores - peak).astype(BF16)
                total = dot(weight, value)
                over = jnp.where(low, total[:half_span, :pair], total[half_span:, :pair])
                under = jnp.where(low, total[:half_span, pair:], total[half_span:, pair:])
                heads[index, rows, column : column + pair] = over / under

    def mlp(block, parts, first=False):
        slots = []
        for at, which in parts:
            for start in (which * size, half_span + which * size):
                slots.append((2 * block + at, slice(start, start + size)))
        gathered = jnp.concatenate([heads[index, rows, :] for index, rows in slots], axis=0)
        if first:
            weights[block * 4 + 1].wait()
        h = jnp.concatenate([xs[index, rows, :] for index, rows in slots], axis=0)
        h = h + dot(gathered.astype(BF16), wproj[block])
        n2 = normed(h, g2_ref[block : block + 1, :])
        if first:
            weights[block * 4 + 2].wait()
            weights[block * 4 + 3].wait()
        count = h.shape[0]
        for column in range(0, hidden, step):
            inner[:count, column : column + step] = gelu(
                dot(n2, wup[block, :, column : column + step]).astype(BF16)
            )
        h = h + dot(inner[:count, :], wdown[block])
        results = []
        for start in range(0, count, 2 * size):
            one, two = h[start : start + size], h[start + size : start + 2 * size]
            results.append(from_pairs(block, one[:piece], two[:piece]))
            results.append(from_pairs(block, one[piece:], two[piece:]))
        return results

    def prepare_first(u):
        atoms = (4 * u, 4 * u + 2, 4 * u + 1, 4 * u + 3)
        prepare(0, u, [x_ref[a] for a in atoms], [e_ref[a] for a in atoms])

    prepare_first(0)
    weights[2].start()
    weights[3].start()
    attend(0, 0)
    own[0], own[2] = mlp(0, [(0, 0)], True)
    pl.semaphore_wait(barrier, 6)
    for at in range(5):
        label_copy(at).start()
    forward_copy(0).start()
    forward_copy(1).start()
    for at in range(4, 8):
        weights[at].start()
    prepare_first(1)
    attend(0, 1)
    own[4], own[6] = mlp(0, [(1, 0)])
    forward_copy(2).start()
    forward_copy(3).start()
    own[1], own[3], own[5], own[7] = mlp(0, [(0, 1), (1, 1)])
    forward_copy(4).start()

    def prepare_second(w):
        pieces, marks = [], []
        for place in range(4):
            if (w, place) in arrivals:
                label_copy(arrivals[w, place]).wait_recv()
                forward_copy(arrivals[w, place]).wait_recv()
        for place in range(4):
            if (w, place) in arrivals:
                pieces.append(shift[w, place])
                marks.append(eshift[w, place])
            else:
                pieces.append(own[local[w, place]])
                marks.append(e_ref[local[w, place]])
        prepare(1, w, pieces, marks)

    def mlp_second(parts, first=False):
        results = mlp(1, parts, first)
        places = [(w, 2 * which + at) for w, which in parts for at in range(2)]
        for (w, place), result in zip(places, results):
            if (w, place) in local:
                out_ref[local[w, place]] = result
            else:
                back[w, place] = result
        for w, place in places:
            if (w, place) in arrivals:
                backward_copy(arrivals[w, place]).start()

    prepare_second(0)
    attend(1, 0)
    mlp_second([(0, 0)], True)
    prepare_second(1)
    attend(1, 1)
    mlp_second([(1, 0)])
    mlp_second([(1, 1), (0, 1)])
    for at in range(5):
        backward_copy(at).wait_recv()
    for at in range(5):
        label_copy(at).wait_send()
        forward_copy(at).wait_send()
        backward_copy(at).wait_send()


def to_atoms(field):
    levels, row_count, column_count = field.shape[:3]
    trailing = tuple(field.shape[3:])
    half_row, half_column = WLAT // 2, WLON // 2
    shaped = field.reshape(
        (levels, row_count // half_row, half_row, column_count // half_column, half_column)
        + trailing
    )
    order = (1, 3, 0, 2, 4) + tuple(range(5, 5 + len(trailing)))
    return jnp.transpose(shaped, order).reshape(
        (-1, levels * half_row * half_column) + trailing
    )


def from_atoms(atoms, levels, row_count, column_count):
    trailing = tuple(atoms.shape[2:])
    half_row, half_column = WLAT // 2, WLON // 2
    shaped = atoms.reshape(
        (row_count // half_row, column_count // half_column, levels, half_row, half_column)
        + trailing
    )
    order = (2, 0, 3, 1, 4) + tuple(range(5, 5 + len(trailing)))
    return jnp.transpose(shaped, order).reshape((levels, row_count, column_count) + trailing)


def per_device(
    tokens, region, norm_gain1, qkv_weight, proj_weight, norm_gain2, up_weight, down_weight
):
    levels, row_count, column_count, features = tokens.shape
    hidden = up_weight.shape[2]
    x = to_atoms(tokens)
    atoms, size, _ = x.shape
    span = 4 * size

    level = jnp.arange(levels, dtype=jnp.int32)[:, None, None]
    row = (lax.axis_index("lat") * row_count + jnp.arange(row_count, dtype=jnp.int32))[None, :, None]
    pair_first = level // WLEV
    rolled_level = (level + levels - WLEV // 2) % levels
    wrapped_level = (rolled_level >= levels - WLEV // 2).astype(jnp.int32)
    wrapped_row = (row < WLAT // 2).astype(jnp.int32)
    first_class = region * 2 + pair_first
    second_class = ((region * 2 + rolled_level // WLEV) * 2 + wrapped_level) * 2 + wrapped_row
    classes = jnp.stack([first_class, second_class + 64], axis=-1)
    classes = to_atoms(classes)
    lane = jnp.arange(128, dtype=jnp.int32)
    marks = (
        (classes[:, :, :1] == lane) | (classes[:, :, 1:] == lane)
    ).astype(BF16)

    vmem = pl.BlockSpec(memory_space=pltpu.VMEM)
    hbm = pl.BlockSpec(memory_space=pl.ANY)
    out = pl.pallas_call(
        kernel,
        out_shape=jax.ShapeDtypeStruct((atoms, size, features), BF16),
        in_specs=[vmem] * 4 + [hbm] * 4,
        out_specs=vmem,
        scratch_shapes=[
            pltpu.VMEM((atoms, size, features), BF16),
            pltpu.VMEM((2, 4, size, features), BF16),
            pltpu.VMEM((2, 4, size, features), BF16),
            pltpu.VMEM((2, 4, size, 128), BF16),
            pltpu.VMEM((4, span, features), F32),
            pltpu.VMEM((4, span, 3 * features), BF16),
            pltpu.VMEM((4, span, features), F32),
            pltpu.VMEM((4, span, 128), BF16),
            pltpu.VMEM((4, span, 128), BF16),
            pltpu.VMEM((span, hidden), BF16),
            pltpu.VMEM(qkv_weight.shape, BF16),
            pltpu.VMEM(proj_weight.shape, BF16),
            pltpu.VMEM(up_weight.shape, BF16),
            pltpu.VMEM(down_weight.shape, BF16),
            pltpu.SemaphoreType.DMA((8,)),
            pltpu.SemaphoreType.DMA((5,)),
            pltpu.SemaphoreType.DMA((5,)),
            pltpu.SemaphoreType.DMA((5,)),
            pltpu.SemaphoreType.DMA((5,)),
            pltpu.SemaphoreType.DMA((5,)),
            pltpu.SemaphoreType.DMA((5,)),
        ],
        compiler_params=pltpu.CompilerParams(
            collective_id=0, has_side_effects=True, vmem_limit_bytes=50 * 1024 * 1024
        ),
    )(x, marks, norm_gain1, norm_gain2, qkv_weight, proj_weight, up_weight, down_weight)
    return from_atoms(out, levels, row_count, column_count)


def solution(mesh):
    return jax.shard_map(
        per_device,
        mesh=mesh,
        in_specs=(P(None, "lat", "lon", None), P(None, "lat", "lon"), P(), P(), P(), P(), P(), P()),
        out_specs=P(None, "lat", "lon", None),
        check_vma=False,
    )
```

```python
import jax
import jax.numpy as jnp
import numpy as np
from jax import lax
from jax.experimental import pallas as pl
from jax.experimental.pallas import tpu as pltpu
from jax.sharding import PartitionSpec as P

HEADS = 8
WLEV = 2
WLAT = 6
WLON = 12
EPSILON = 1e-05
FAR = -1e30
LANES = 128
MESH = pl.DeviceIdType.MESH
F32 = jnp.float32
BF16 = jnp.bfloat16


def normed(field, gain):
    mean = jnp.mean(field, axis=-1, keepdims=True)
    centered = field - mean
    variance = jnp.mean(centered * centered, axis=-1, keepdims=True)
    return (centered * lax.rsqrt(variance + EPSILON) * gain).astype(BF16)


def gelu(x):
    inner = x * (0.7978845608028654 + 0.035677408136300125 * (x * x))
    half = 0.5 * x
    return half + half * jnp.tanh(inner)


def dot(a, b):
    return jnp.dot(a, b, preferred_element_type=F32)


def dot_t(a, b):
    return lax.dot_general(a, b, (((1,), (1,)), ((), ())), preferred_element_type=F32)


HALF_ROW, HALF_COLUMN = WLAT // 2, WLON // 2
CELL = HALF_ROW * HALF_COLUMN
QUARTER = WLEV * CELL
SPOT = 16


def label_tables(levels):
    windows = levels // WLEV
    select = np.zeros((2, windows * 4 * QUARTER, LANES), np.float32)
    column = np.zeros((windows * 4 * QUARTER, LANES), np.float32)
    rows = 4 * HALF_ROW * levels
    for block in range(2):
        for token in range(select.shape[1]):
            group, rest = divmod(token, 4 * QUARTER)
            place, rest = divmod(rest, QUARTER)
            spot, level = divmod(rest, WLEV)
            row, col = divmod(spot, HALF_COLUMN)
            level = (group * WLEV + level + block * (WLEV // 2)) % levels
            select[block, token, (place * HALF_ROW + row) * levels + level] = 1
            column[token, col + HALF_COLUMN * (place // 2)] = 1
            column[token, SPOT] = 1
            if block == 1:
                select[block, token, rows] = level < WLEV // 2
                select[block, token, rows + 1] = place in (1, 2)
    return jnp.asarray(select, BF16), jnp.asarray(column, F32)


def kernel(
    x_hbm, e_hbm, select_hbm, column_hbm, g1_hbm, g2_hbm,
    wqkv_hbm, wproj_hbm, wup_hbm, wdown_hbm, out_ref,
    xin, region, select, column, g1, g2, regions, own, shift, side, corner, below,
    xs, qkv, heads, marks_q, marks_k, inner, flat, cross, wide, ready, o_send, o_back,
    wqkv, wproj, wup, wdown, wsem, isem, fsend, frecv, esend, erecv, osend, orecv, bsend, brecv,
):
    lat_count, lon_count = lax.axis_size("lat"), lax.axis_size("lon")
    lat, lon = lax.axis_index("lat"), lax.axis_index("lon")
    up = lax.rem(lat + lat_count - 1, lat_count)
    down = lax.rem(lat + 1, lat_count)
    left = lax.rem(lon + lon_count - 1, lon_count)
    right = lax.rem(lon + 1, lon_count)
    before = {"left": (lat, left), "up": (up, lon), "corner": (up, left)}
    after = {"left": (lat, right), "up": (down, lon), "corner": (down, right)}

    spots, lane_tiles, levels, lanes = xin.shape
    features = lane_tiles * lanes
    span = xs.shape[1]
    group = span // 2
    half = group // 2
    hidden = wup.shape[2]
    step = 256
    columns = 2 * HALF_COLUMN
    window_spots = spots // 2

    weights = [
        pltpu.make_async_copy(source.at[block], target.at[block], wsem.at[block * 4 + at])
        for block in range(2)
        for at, (source, target) in enumerate(
            ((wqkv_hbm, wqkv), (wproj_hbm, wproj), (wup_hbm, wup), (wdown_hbm, wdown))
        )
    ]
    halves = [pl.ds(u * window_spots, window_spots) for u in range(2)]
    inputs = [
        pltpu.make_async_copy(source, target, isem.at[at])
        for at, (source, target) in enumerate(
            (
                (x_hbm.at[halves[0]], xin.at[halves[0]]),
                (x_hbm.at[halves[1]], xin.at[halves[1]]),
                (e_hbm, region),
                (select_hbm, select),
                (column_hbm, column),
                (g1_hbm, g1),
                (g2_hbm, g2),
            )
        )
    ]
    inputs[0].start()
    for at in (5, 2, 3, 4):
        inputs[at].start()
    weights[0].start()
    inputs[1].start()
    inputs[6].start()
    for at in range(1, 4):
        weights[at].start()

    barrier = pltpu.get_barrier_semaphore()
    for device in list(before.values()) + list(after.values()):
        pl.semaphore_signal(barrier, inc=1, device_id=device, device_id_type=MESH)

    moves = (
        (2, 0, 0, "left"),
        (0, 1, 1, "corner"),
        (4, 0, 1, "left"),
        (6, 1, 0, "left"),
        (1, 1, 2, "up"),
    )
    local = {(0, 2): 3, (0, 3): 5, (1, 3): 7}
    arrivals = {(move[1], move[2]): at for at, move in enumerate(moves)}
    returns = ((6, 0, "left"), (0, 1, "corner"), (1, 2, "up"))

    def remote(source, target, send, recv, device):
        return pltpu.make_async_remote_copy(
            source, target, send, recv, device_id=device, device_id_type=MESH
        )

    labels = [
        remote(region.at[HALF_ROW:], side, esend.at[0], erecv.at[0], before["left"]),
        remote(region.at[:HALF_ROW], corner, esend.at[1], erecv.at[1], before["corner"]),
        remote(region.at[:HALF_ROW], below, esend.at[2], erecv.at[2], before["up"]),
    ]
    forward = [
        remote(own.at[atom], shift.at[window, place], fsend.at[at], frecv.at[at], before[towards])
        for at, (atom, window, place, towards) in enumerate(moves)
    ]
    outward = remote(o_send, o_back, osend.at[0], orecv.at[0], after["left"])

    def first_spot(atom, row):
        return ((atom // 2) * HALF_ROW + row) * columns + (atom % 2) * HALF_COLUMN

    backward = [
        remote(
            ready.at[at, pl.ds(row * HALF_COLUMN, HALF_COLUMN)],
            out_ref.at[pl.ds(first_spot(atom, row), HALF_COLUMN)],
            bsend.at[at * HALF_ROW + row],
            brecv.at[at * HALF_ROW + row],
            after[towards],
        )
        for at, (atom, place, towards) in enumerate(returns)
        for row in range(HALF_ROW)
    ]

    lane = lax.broadcasted_iota(jnp.int32, (1, lanes), 1)
    lane_value = lane.astype(F32)
    low = lane < 64
    scale = 64 ** -0.5
    head_masks = (
        jnp.where(low, scale, 0.0).astype(BF16),
        jnp.where(low, 0.0, scale).astype(BF16),
    )

    def tile(at):
        return slice(at * lanes, (at + 1) * lanes)

    def mark(block, at, places):
        index = 2 * block + at
        count = HALF_ROW * levels
        regions[index] = jnp.zeros(regions.shape[1:], F32)
        for place, (source, row) in enumerate(places):
            for r in range(HALF_ROW):
                start = place * count + r * levels
                regions[index, start : start + levels, :columns] = source[row + r].astype(F32)
        if block == 1:
            wrapped = jnp.where(lat == lat_count - 1, 8.0, 0.0) if at == 1 else 0.0
            regions[index, 4 * count : 4 * count + 1, :] = jnp.where(lane == SPOT, 4.0, 0.0)
            regions[index, 4 * count + 1 : 4 * count + 2, :] = jnp.where(lane == SPOT, wrapped, 0.0)
        value = dot(select[block], regions[index].astype(BF16)) * column[...]
        same = jnp.sum(value, axis=-1, keepdims=True) == lane_value
        marks_q[index] = jnp.where(same, FAR, 0.0).astype(BF16)
        marks_k[index] = jnp.where(same, 0.0, 1.0).astype(BF16)

    def project(block, at):
        index = 2 * block + at
        n1 = normed(xs[index], g1[block : block + 1, :])
        if at == 0:
            weights[block * 4].wait()
        qkv[index] = dot(n1, wqkv[block]).astype(BF16)

    cut = -(-half // 16) * 16

    def attend(block, at, which):
        index = 2 * block + at
        first, last = ((0, cut), (cut, group), (0, group))[which]
        size = last - first
        ones = jnp.ones((group, lanes), BF16)
        for start in (0, group):
            rows = slice(start + first, start + last)
            keys = slice(start, start + group)
            mark_q = marks_q[index, rows, :]
            mark_q = jnp.concatenate([mark_q, mark_q], axis=0)
            mark_k = marks_k[index, keys, :]
            for at_tile in range(lane_tiles):
                query = qkv[index, rows, tile(at_tile)]
                key = qkv[index, keys, tile(lane_tiles + at_tile)]
                value = qkv[index, keys, tile(2 * lane_tiles + at_tile)]
                value = jnp.concatenate([value, ones], axis=1)
                query = jnp.concatenate([query * head_masks[0], query * head_masks[1]], axis=0)
                scores = dot_t(
                    jnp.concatenate([query, mark_q], axis=1),
                    jnp.concatenate([key, mark_k], axis=1),
                )
                peak = jnp.max(scores, axis=-1, keepdims=True)
                weight = jnp.exp(scores - peak).astype(BF16)
                total = dot(weight, value)
                over = jnp.where(low, total[:size, :lanes], total[size:, :lanes])
                under = jnp.where(low, total[:size, lanes:], total[size:, lanes:])
                heads[index, rows, tile(at_tile)] = over / under

    def gather(source, parts):
        pieces = []
        for index, which in parts:
            for start in (which * half, group + which * half):
                pieces.append(source[index, start : start + half, :])
        return jnp.concatenate(pieces, axis=0)

    def mlp(block, h, mixed, first=False):
        if first:
            weights[block * 4 + 1].wait()
        h = h + dot(mixed, wproj[block])
        n2 = normed(h, g2[block : block + 1, :])
        if first:
            weights[block * 4 + 2].wait()
        count = h.shape[0]
        for at in range(0, hidden, step):
            inner[:count, at : at + step] = gelu(
                dot(n2, wup[block, :, at : at + step]).astype(BF16)
            )
        if first:
            weights[block * 4 + 3].wait()
        return h + dot(inner[:count, :], wdown[block])

    def relevel(slot, h, shifts, targets, stride):
        for at in range(lane_tiles):
            flat[slot, at] = h[:, tile(at)]
        for place, target in enumerate(targets):
            for at in range(lane_tiles):
                for group_at in range(2):
                    for lev in range(WLEV):
                        source = group_at * half + place * QUARTER + lev
                        target[at, pl.ds(shifts[group_at][lev], CELL, stride=stride)] = flat[
                            slot, at, pl.ds(source, CELL, stride=WLEV)
                        ]

    def finish_first(slot, h, atoms):
        targets = [cross.at[slot, place] for place in range(2)]
        relevel(slot, h, ((QUARTER + 1, 0), (1, QUARTER)), targets, WLEV)
        for place, atom in enumerate(atoms):
            for at in range(lane_tiles):
                own[atom, :, tile(at)] = cross[slot, place, at].astype(BF16)

    def finish_second(slot, h, results):
        targets = [wide.at[slot, place] for place in range(2)]
        relevel(slot, h, ((1, 2), (3, 0)), targets, levels)
        for place, result in enumerate(results):
            for spot in range(CELL):
                row, col = divmod(spot, HALF_COLUMN)
                for at in range(lane_tiles):
                    value = wide[slot, place, at, spot * levels : (spot + 1) * levels].astype(BF16)
                    if result[0] == "out":
                        out_ref[first_spot(result[1], row) + col, at] = value
                    else:
                        ready[result[1], spot, at] = value
            if result[0] == "send":
                for row in range(HALF_ROW):
                    backward[result[1] * HALF_ROW + row].start()

    def load_first(u):
        inputs[u].wait()
        for spot in range(window_spots):
            row, col = divmod(spot, columns)
            place = (col // HALF_COLUMN) * 2 + row // HALF_ROW
            at_spot = (row % HALF_ROW) * HALF_COLUMN + col % HALF_COLUMN
            start = place * QUARTER + at_spot * WLEV
            for at in range(lane_tiles):
                value = xin[u * window_spots + spot, at].astype(F32)
                for group_at in range(2):
                    xs[u, group_at * group + start : group_at * group + start + WLEV, tile(at)] = (
                        value[group_at * WLEV : (group_at + 1) * WLEV]
                    )

    def own_regions(u):
        places = [(region, u * WLAT), (region, u * WLAT + HALF_ROW)]
        return places + places

    def load_second(w, places):
        for place in places:
            if (w, place) in arrivals:
                forward[arrivals[w, place]].wait_recv()
                value = shift[w, place].astype(F32)
            else:
                value = own[local[w, place]].astype(F32)
            for group_at in range(2):
                start = group_at * group + place * QUARTER
                xs[2 + w, start : start + QUARTER, :] = value[
                    group_at * QUARTER : (group_at + 1) * QUARTER
                ]

    load_first(0)
    inputs[2].wait()
    inputs[3].wait()
    inputs[4].wait()
    mark(0, 0, own_regions(0))
    inputs[5].wait()
    project(0, 0)
    pl.semaphore_wait(barrier, 6)
    for copy in labels:
        copy.start()
    for at in range(4, 8):
        weights[at].start()
    attend(0, 0, 0)
    inputs[6].wait()
    h = mlp(0, gather(xs, [(0, 0)]), gather(heads, [(0, 0)]).astype(BF16), True)
    finish_first(0, h, (0, 2))
    forward[0].start()
    forward[1].start()
    load_first(1)
    mark(0, 1, own_regions(1))
    project(0, 1)
    attend(0, 1, 0)
    h = mlp(0, gather(xs, [(1, 0)]), gather(heads, [(1, 0)]).astype(BF16))
    finish_first(1, h, (4, 6))
    forward[2].start()
    forward[3].start()
    attend(0, 0, 1)
    attend(0, 1, 1)
    parts = [(0, 1), (1, 1)]
    h = mlp(0, gather(xs, parts), gather(heads, parts).astype(BF16))
    finish_first(0, h[:group], (1, 3))
    forward[4].start()
    finish_first(1, h[group:], (5, 7))

    for copy in labels:
        copy.wait_recv()
    load_second(0, (2, 3))
    mark(1, 0, [(side, 0), (side, HALF_ROW), (region, HALF_ROW), (region, 2 * HALF_ROW)])
    mark(1, 1, [(side, 2 * HALF_ROW), (corner, 0), (below, 0), (region, 3 * HALF_ROW)])
    load_second(0, (0, 1))
    project(1, 0)
    attend(1, 0, 0)
    o_send[...] = gather(heads, [(2, 0)]).astype(BF16)
    outward.start()
    attend(1, 0, 1)
    load_second(1, (0, 1, 2, 3))
    project(1, 1)
    attend(1, 1, 0)
    h = mlp(1, gather(xs, [(3, 0)]), gather(heads, [(3, 0)]).astype(BF16), True)
    finish_second(0, h, (("send", 0), ("send", 1)))
    attend(1, 1, 1)
    parts = [(3, 1), (2, 1)]
    h = mlp(1, gather(xs, parts), gather(heads, parts).astype(BF16))
    finish_second(1, h[:group], (("send", 2), ("out", 7)))
    finish_second(0, h[group:], (("out", 3), ("out", 5)))
    pieces = [own[2].astype(F32), own[4].astype(F32)]
    residual = jnp.concatenate(
        [piece[:QUARTER] for piece in pieces] + [piece[QUARTER:] for piece in pieces], axis=0
    )
    outward.wait_recv()
    h = mlp(1, residual, o_back[...])
    finish_second(1, h, (("out", 2), ("out", 4)))
    for copy in backward:
        copy.wait_recv()
    for copy in labels + forward + [outward] + backward:
        copy.wait_send()


def per_device(
    tokens, region, norm_gain1, qkv_weight, proj_weight, norm_gain2, up_weight, down_weight
):
    levels, row_count, column_count, features = tokens.shape
    hidden = up_weight.shape[2]
    lane_tiles = features // LANES
    spots = row_count * column_count
    quarter_rows = levels * CELL
    span = 4 * quarter_rows
    group = span // 2
    x = jnp.transpose(tokens.reshape(levels, spots, lane_tiles, LANES), (1, 2, 0, 3))
    marks = jnp.transpose(region, (1, 0, 2))
    select, column = label_tables(levels)

    vmem = pl.BlockSpec(memory_space=pltpu.VMEM)
    hbm = pl.BlockSpec(memory_space=pl.ANY)
    dma = pltpu.SemaphoreType.DMA
    out = pl.pallas_call(
        kernel,
        out_shape=jax.ShapeDtypeStruct(x.shape, BF16),
        in_specs=[hbm] * 10,
        out_specs=vmem,
        scratch_shapes=[
            pltpu.VMEM(x.shape, BF16),
            pltpu.VMEM(marks.shape, jnp.int32),
            pltpu.VMEM(select.shape, BF16),
            pltpu.VMEM(column.shape, F32),
            pltpu.VMEM(norm_gain1.shape, F32),
            pltpu.VMEM(norm_gain2.shape, F32),
            pltpu.VMEM((4, LANES, LANES), F32),
            pltpu.VMEM((8, quarter_rows, features), BF16),
            pltpu.VMEM((2, 4, quarter_rows, features), BF16),
            pltpu.VMEM((row_count - HALF_ROW,) + marks.shape[1:], jnp.int32),
            pltpu.VMEM((HALF_ROW,) + marks.shape[1:], jnp.int32),
            pltpu.VMEM((HALF_ROW,) + marks.shape[1:], jnp.int32),
            pltpu.VMEM((4, span, features), F32),
            pltpu.VMEM((4, span, 3 * features), BF16),
            pltpu.VMEM((4, span, features), F32),
            pltpu.VMEM((4, span, LANES), BF16),
            pltpu.VMEM((4, span, LANES), BF16),
            pltpu.VMEM((span, hidden), BF16),
            pltpu.VMEM((2, lane_tiles, group, LANES), F32),
            pltpu.VMEM((2, 2, lane_tiles, quarter_rows, LANES), F32),
            pltpu.VMEM((2, 2, lane_tiles, quarter_rows, LANES), F32),
            pltpu.VMEM((3, CELL) + x.shape[1:], BF16),
            pltpu.VMEM((group, features), BF16),
            pltpu.VMEM((group, features), BF16),
            pltpu.VMEM(qkv_weight.shape, BF16),
            pltpu.VMEM(proj_weight.shape, BF16),
            pltpu.VMEM(up_weight.shape, BF16),
            pltpu.VMEM(down_weight.shape, BF16),
            dma((8,)),
            dma((7,)),
            dma((5,)),
            dma((5,)),
            dma((3,)),
            dma((3,)),
            dma((1,)),
            dma((1,)),
            dma((3 * HALF_ROW,)),
            dma((3 * HALF_ROW,)),
        ],
        compiler_params=pltpu.CompilerParams(
            collective_id=0, has_side_effects=True, vmem_limit_bytes=56 * 1024 * 1024
        ),
    )(
        x, marks, select, column, norm_gain1, norm_gain2,
        qkv_weight, proj_weight, up_weight, down_weight,
    )
    return jnp.transpose(out, (2, 0, 1, 3)).reshape(tokens.shape)


def solution(mesh):
    return jax.shard_map(
        per_device,
        mesh=mesh,
        in_specs=(P(None, "lat", "lon", None), P(None, "lat", "lon"), P(), P(), P(), P(), P(), P()),
        out_specs=P(None, "lat", "lon", None),
        check_vma=False,
    )
```

```python
import jax
import jax.numpy as jnp
import numpy as np
from jax import lax
from jax.experimental import pallas as pl
from jax.experimental.pallas import tpu as pltpu
from jax.sharding import PartitionSpec as P

HEADS = 8
WLEV = 2
WLAT = 6
WLON = 12
EPSILON = 1e-05
FAR = -1e30
LANES = 128
MESH = pl.DeviceIdType.MESH
F32 = jnp.float32
BF16 = jnp.bfloat16


def normed(field, gain):
    mean = jnp.mean(field, axis=-1, keepdims=True)
    centered = field - mean
    variance = jnp.mean(centered * centered, axis=-1, keepdims=True)
    return (centered * lax.rsqrt(variance + EPSILON) * gain).astype(BF16)


def gelu(x):
    inner = x * (0.7978845608028654 + 0.035677408136300125 * (x * x))
    half = 0.5 * x
    return half + half * jnp.tanh(inner)


def dot(a, b):
    return jnp.dot(a, b, preferred_element_type=F32)


def dot_t(a, b):
    return lax.dot_general(a, b, (((1,), (1,)), ((), ())), preferred_element_type=F32)


HALF_ROW, HALF_COLUMN = WLAT // 2, WLON // 2
CELL = HALF_ROW * HALF_COLUMN
QUARTER = WLEV * CELL
SPOT = 16


def label_tables(levels):
    windows = levels // WLEV
    select = np.zeros((2, windows * 4 * QUARTER, LANES), np.float32)
    column = np.zeros((windows * 4 * QUARTER, LANES), np.float32)
    rows = 4 * HALF_ROW * levels
    for block in range(2):
        for token in range(select.shape[1]):
            group, rest = divmod(token, 4 * QUARTER)
            place, rest = divmod(rest, QUARTER)
            spot, level = divmod(rest, WLEV)
            row, col = divmod(spot, HALF_COLUMN)
            level = (group * WLEV + level + block * (WLEV // 2)) % levels
            select[block, token, (place * HALF_ROW + row) * levels + level] = 1
            column[token, col + HALF_COLUMN * (place // 2)] = 1
            column[token, SPOT] = 1
            if block == 1:
                select[block, token, rows] = level < WLEV // 2
                select[block, token, rows + 1] = place in (1, 2)
    return jnp.asarray(select, BF16), jnp.asarray(column, F32)


def kernel(
    x_hbm, e_hbm, select_hbm, column_hbm, g1_hbm, g2_hbm,
    wqkv_hbm, wproj_hbm, wup_hbm, wdown_hbm, out_ref,
    xin, region, select, column, g1, g2, regions, own, shift, side, corner, below,
    xs, qkv, heads, marks_q, marks_k, inner, flat, cross, wide, ready, o_send, o_back,
    wqkv, wproj, wup, wdown, wsem, isem, fsend, frecv, esend, erecv, osend, orecv, bsend, brecv,
):
    lat_count, lon_count = lax.axis_size("lat"), lax.axis_size("lon")
    lat, lon = lax.axis_index("lat"), lax.axis_index("lon")
    up = lax.rem(lat + lat_count - 1, lat_count)
    down = lax.rem(lat + 1, lat_count)
    left = lax.rem(lon + lon_count - 1, lon_count)
    right = lax.rem(lon + 1, lon_count)
    before = {"left": (lat, left), "up": (up, lon), "corner": (up, left)}
    after = {"left": (lat, right), "up": (down, lon), "corner": (down, right)}

    spots, lane_tiles, levels, lanes = xin.shape
    features = lane_tiles * lanes
    span = xs.shape[1]
    group = span // 2
    half = group // 2
    hidden = wup.shape[2]
    step = 256
    columns = 2 * HALF_COLUMN
    window_spots = spots // 2

    weights = [
        pltpu.make_async_copy(source.at[block], target.at[block], wsem.at[block * 4 + at])
        for block in range(2)
        for at, (source, target) in enumerate(
            ((wqkv_hbm, wqkv), (wproj_hbm, wproj), (wup_hbm, wup), (wdown_hbm, wdown))
        )
    ]
    halves = [pl.ds(u * window_spots, window_spots) for u in range(2)]
    inputs = [
        pltpu.make_async_copy(source, target, isem.at[at])
        for at, (source, target) in enumerate(
            (
                (x_hbm.at[halves[0]], xin.at[halves[0]]),
                (x_hbm.at[halves[1]], xin.at[halves[1]]),
                (e_hbm, region),
                (select_hbm, select),
                (column_hbm, column),
                (g1_hbm, g1),
                (g2_hbm, g2),
            )
        )
    ]
    inputs[0].start()
    for at in (5, 2, 3, 4):
        inputs[at].start()
    weights[0].start()
    inputs[1].start()
    inputs[6].start()
    for at in range(1, 4):
        weights[at].start()

    barrier = pltpu.get_barrier_semaphore()
    for device in list(before.values()) + list(after.values()):
        pl.semaphore_signal(barrier, inc=1, device_id=device, device_id_type=MESH)

    moves = (
        (2, 0, 0, "left"),
        (0, 1, 1, "corner"),
        (4, 0, 1, "left"),
        (6, 1, 0, "left"),
        (1, 1, 2, "up"),
    )
    local = {(0, 2): 3, (0, 3): 5, (1, 3): 7}
    arrivals = {(move[1], move[2]): at for at, move in enumerate(moves)}
    returns = ((6, 0, "left"), (0, 1, "corner"), (1, 2, "up"))

    def remote(source, target, send, recv, device):
        return pltpu.make_async_remote_copy(
            source, target, send, recv, device_id=device, device_id_type=MESH
        )

    labels = [
        remote(region.at[HALF_ROW:], side, esend.at[0], erecv.at[0], before["left"]),
        remote(region.at[:HALF_ROW], corner, esend.at[1], erecv.at[1], before["corner"]),
        remote(region.at[:HALF_ROW], below, esend.at[2], erecv.at[2], before["up"]),
    ]
    forward = [
        remote(own.at[atom], shift.at[window, place], fsend.at[at], frecv.at[at], before[towards])
        for at, (atom, window, place, towards) in enumerate(moves)
    ]
    outward = remote(o_send, o_back, osend.at[0], orecv.at[0], after["left"])

    def first_spot(atom, row):
        return ((atom // 2) * HALF_ROW + row) * columns + (atom % 2) * HALF_COLUMN

    backward = [
        remote(
            ready.at[at, pl.ds(row * HALF_COLUMN, HALF_COLUMN)],
            out_ref.at[pl.ds(first_spot(atom, row), HALF_COLUMN)],
            bsend.at[at * HALF_ROW + row],
            brecv.at[at * HALF_ROW + row],
            after[towards],
        )
        for at, (atom, place, towards) in enumerate(returns)
        for row in range(HALF_ROW)
    ]

    lane = lax.broadcasted_iota(jnp.int32, (1, lanes), 1)
    lane_value = lane.astype(F32)
    low = lane < 64
    scale = 64 ** -0.5
    head_masks = (
        jnp.where(low, scale, 0.0).astype(BF16),
        jnp.where(low, 0.0, scale).astype(BF16),
    )

    def tile(at):
        return slice(at * lanes, (at + 1) * lanes)

    def mark(block, at, places):
        index = 2 * block + at
        count = HALF_ROW * levels
        regions[index] = jnp.zeros(regions.shape[1:], F32)
        for place, (source, row) in enumerate(places):
            for r in range(HALF_ROW):
                start = place * count + r * levels
                regions[index, start : start + levels, :columns] = source[row + r].astype(F32)
        if block == 1:
            wrapped = jnp.where(lat == lat_count - 1, 8.0, 0.0) if at == 1 else 0.0
            regions[index, 4 * count : 4 * count + 1, :] = jnp.where(lane == SPOT, 4.0, 0.0)
            regions[index, 4 * count + 1 : 4 * count + 2, :] = jnp.where(lane == SPOT, wrapped, 0.0)
        value = dot(select[block], regions[index].astype(BF16)) * column[...]
        same = jnp.sum(value, axis=-1, keepdims=True) == lane_value
        marks_q[index] = jnp.where(same, FAR, 0.0).astype(BF16)
        marks_k[index] = jnp.where(same, 0.0, 1.0).astype(BF16)

    def project(block, at):
        index = 2 * block + at
        n1 = normed(xs[index], g1[block : block + 1, :])
        if at == 0:
            weights[block * 4].wait()
        qkv[index] = dot(n1, wqkv[block]).astype(BF16)

    def attend(block, at):
        index = 2 * block + at
        ones = jnp.ones((group, lanes), BF16)
        for start in (0, group):
            rows = slice(start, start + group)
            mark_q = marks_q[index, rows, :]
            mark_q = jnp.concatenate([mark_q, mark_q], axis=0)
            mark_k = marks_k[index, rows, :]
            for at_tile in range(lane_tiles):
                query = qkv[index, rows, tile(at_tile)]
                key = qkv[index, rows, tile(lane_tiles + at_tile)]
                value = qkv[index, rows, tile(2 * lane_tiles + at_tile)]
                value = jnp.concatenate([value, ones], axis=1)
                query = jnp.concatenate([query * head_masks[0], query * head_masks[1]], axis=0)
                scores = dot_t(
                    jnp.concatenate([query, mark_q], axis=1),
                    jnp.concatenate([key, mark_k], axis=1),
                )
                peak = jnp.max(scores, axis=-1, keepdims=True)
                weight = jnp.exp(scores - peak).astype(BF16)
                total = dot(weight, value)
                over = jnp.where(low, total[:group, :lanes], total[group:, :lanes])
                under = jnp.where(low, total[:group, lanes:], total[group:, lanes:])
                heads[index, rows, tile(at_tile)] = over / under

    def gather(source, parts):
        pieces = []
        for index, which in parts:
            for start in (which * half, group + which * half):
                pieces.append(source[index, start : start + half, :])
        return jnp.concatenate(pieces, axis=0)

    def mlp(block, h, mixed, first=False):
        if first:
            weights[block * 4 + 1].wait()
        h = h + dot(mixed, wproj[block])
        n2 = normed(h, g2[block : block + 1, :])
        if first:
            weights[block * 4 + 2].wait()
        count = h.shape[0]
        for at in range(0, hidden, step):
            inner[:count, at : at + step] = gelu(
                dot(n2, wup[block, :, at : at + step]).astype(BF16)
            )
        if first:
            weights[block * 4 + 3].wait()
        return h + dot(inner[:count, :], wdown[block])

    def relevel(slot, h, shifts, targets, stride):
        for at in range(lane_tiles):
            flat[slot, at] = h[:, tile(at)]
        for place, target in enumerate(targets):
            for at in range(lane_tiles):
                for group_at in range(2):
                    for lev in range(WLEV):
                        source = group_at * half + place * QUARTER + lev
                        target[at, pl.ds(shifts[group_at][lev], CELL, stride=stride)] = flat[
                            slot, at, pl.ds(source, CELL, stride=WLEV)
                        ]

    def finish_first(slot, h, atoms):
        targets = [cross.at[slot, place] for place in range(2)]
        relevel(slot, h, ((QUARTER + 1, 0), (1, QUARTER)), targets, WLEV)
        for place, atom in enumerate(atoms):
            for at in range(lane_tiles):
                own[atom, :, tile(at)] = cross[slot, place, at].astype(BF16)

    def finish_second(slot, h, results):
        targets = [wide.at[slot, place] for place in range(2)]
        relevel(slot, h, ((1, 2), (3, 0)), targets, levels)
        for place, result in enumerate(results):
            for spot in range(CELL):
                row, col = divmod(spot, HALF_COLUMN)
                for at in range(lane_tiles):
                    value = wide[slot, place, at, spot * levels : (spot + 1) * levels].astype(BF16)
                    if result[0] == "out":
                        out_ref[first_spot(result[1], row) + col, at] = value
                    else:
                        ready[result[1], spot, at] = value
            if result[0] == "send":
                for row in range(HALF_ROW):
                    backward[result[1] * HALF_ROW + row].start()

    def load_first(u):
        inputs[u].wait()
        for spot in range(window_spots):
            row, col = divmod(spot, columns)
            place = (col // HALF_COLUMN) * 2 + row // HALF_ROW
            at_spot = (row % HALF_ROW) * HALF_COLUMN + col % HALF_COLUMN
            start = place * QUARTER + at_spot * WLEV
            for at in range(lane_tiles):
                value = xin[u * window_spots + spot, at].astype(F32)
                for group_at in range(2):
                    xs[u, group_at * group + start : group_at * group + start + WLEV, tile(at)] = (
                        value[group_at * WLEV : (group_at + 1) * WLEV]
                    )

    def own_regions(u):
        places = [(region, u * WLAT), (region, u * WLAT + HALF_ROW)]
        return places + places

    def load_second(w, places):
        for place in places:
            if (w, place) in arrivals:
                forward[arrivals[w, place]].wait_recv()
                value = shift[w, place].astype(F32)
            else:
                value = own[local[w, place]].astype(F32)
            for group_at in range(2):
                start = group_at * group + place * QUARTER
                xs[2 + w, start : start + QUARTER, :] = value[
                    group_at * QUARTER : (group_at + 1) * QUARTER
                ]

    load_first(0)
    inputs[2].wait()
    inputs[3].wait()
    inputs[4].wait()
    mark(0, 0, own_regions(0))
    inputs[5].wait()
    project(0, 0)
    pl.semaphore_wait(barrier, 6)
    for copy in labels:
        copy.start()
    for at in range(4, 8):
        weights[at].start()
    attend(0, 0)
    inputs[6].wait()
    h = mlp(0, gather(xs, [(0, 0)]), gather(heads, [(0, 0)]).astype(BF16), True)
    finish_first(0, h, (0, 2))
    forward[0].start()
    forward[1].start()
    load_first(1)
    mark(0, 1, own_regions(1))
    project(0, 1)
    attend(0, 1)
    h = mlp(0, gather(xs, [(1, 0)]), gather(heads, [(1, 0)]).astype(BF16))
    finish_first(1, h, (4, 6))
    forward[2].start()
    forward[3].start()
    parts = [(0, 1), (1, 1)]
    h = mlp(0, gather(xs, parts), gather(heads, parts).astype(BF16))
    finish_first(0, h[:group], (1, 3))
    forward[4].start()
    finish_first(1, h[group:], (5, 7))

    for copy in labels:
        copy.wait_recv()
    load_second(0, (2, 3))
    mark(1, 0, [(side, 0), (side, HALF_ROW), (region, HALF_ROW), (region, 2 * HALF_ROW)])
    mark(1, 1, [(side, 2 * HALF_ROW), (corner, 0), (below, 0), (region, 3 * HALF_ROW)])
    load_second(0, (0, 1))
    project(1, 0)
    attend(1, 0)
    o_send[...] = gather(heads, [(2, 0)]).astype(BF16)
    outward.start()
    load_second(1, (0, 1, 2, 3))
    project(1, 1)
    attend(1, 1)
    h = mlp(1, gather(xs, [(3, 0)]), gather(heads, [(3, 0)]).astype(BF16), True)
    finish_second(0, h, (("send", 0), ("send", 1)))
    parts = [(3, 1), (2, 1)]
    h = mlp(1, gather(xs, parts), gather(heads, parts).astype(BF16))
    finish_second(1, h[:group], (("send", 2), ("out", 7)))
    finish_second(0, h[group:], (("out", 3), ("out", 5)))
    pieces = [own[2].astype(F32), own[4].astype(F32)]
    residual = jnp.concatenate(
        [piece[:QUARTER] for piece in pieces] + [piece[QUARTER:] for piece in pieces], axis=0
    )
    outward.wait_recv()
    h = mlp(1, residual, o_back[...])
    finish_second(1, h, (("out", 2), ("out", 4)))
    for copy in backward:
        copy.wait_recv()
    for copy in labels + forward + [outward] + backward:
        copy.wait_send()


def settle(source, target, sems):
    chunks = sems.shape[0]
    size = source.shape[0] // chunks
    copies = [
        pltpu.make_async_copy(
            source.at[pl.ds(at * size, size)], target.at[pl.ds(at * size, size)], sems.at[at]
        )
        for at in range(chunks)
    ]
    for copy in copies:
        copy.start()
    for copy in copies:
        copy.wait()


def per_device(
    tokens, region, norm_gain1, qkv_weight, proj_weight, norm_gain2, up_weight, down_weight
):
    levels, row_count, column_count, features = tokens.shape
    hidden = up_weight.shape[2]
    lane_tiles = features // LANES
    spots = row_count * column_count
    quarter_rows = levels * CELL
    span = 4 * quarter_rows
    group = span // 2
    x = jnp.transpose(tokens.reshape(levels, spots, lane_tiles, LANES), (1, 2, 0, 3))
    marks = jnp.transpose(region, (1, 0, 2))
    select, column = label_tables(levels)

    vmem = pl.BlockSpec(memory_space=pltpu.VMEM)
    hbm = pl.BlockSpec(memory_space=pl.ANY)
    dma = pltpu.SemaphoreType.DMA
    out = pl.pallas_call(
        kernel,
        out_shape=pltpu.VMEM(x.shape, BF16),
        in_specs=[hbm] * 10,
        out_specs=vmem,
        scratch_shapes=[
            pltpu.VMEM(x.shape, BF16),
            pltpu.VMEM(marks.shape, jnp.int32),
            pltpu.VMEM(select.shape, BF16),
            pltpu.VMEM(column.shape, F32),
            pltpu.VMEM(norm_gain1.shape, F32),
            pltpu.VMEM(norm_gain2.shape, F32),
            pltpu.VMEM((4, LANES, LANES), F32),
            pltpu.VMEM((8, quarter_rows, features), BF16),
            pltpu.VMEM((2, 4, quarter_rows, features), BF16),
            pltpu.VMEM((row_count - HALF_ROW,) + marks.shape[1:], jnp.int32),
            pltpu.VMEM((HALF_ROW,) + marks.shape[1:], jnp.int32),
            pltpu.VMEM((HALF_ROW,) + marks.shape[1:], jnp.int32),
            pltpu.VMEM((4, span, features), F32),
            pltpu.VMEM((4, span, 3 * features), BF16),
            pltpu.VMEM((4, span, features), F32),
            pltpu.VMEM((4, span, LANES), BF16),
            pltpu.VMEM((4, span, LANES), BF16),
            pltpu.VMEM((span, hidden), BF16),
            pltpu.VMEM((2, lane_tiles, group, LANES), F32),
            pltpu.VMEM((2, 2, lane_tiles, quarter_rows, LANES), F32),
            pltpu.VMEM((2, 2, lane_tiles, quarter_rows, LANES), F32),
            pltpu.VMEM((3, CELL) + x.shape[1:], BF16),
            pltpu.VMEM((group, features), BF16),
            pltpu.VMEM((group, features), BF16),
            pltpu.VMEM(qkv_weight.shape, BF16),
            pltpu.VMEM(proj_weight.shape, BF16),
            pltpu.VMEM(up_weight.shape, BF16),
            pltpu.VMEM(down_weight.shape, BF16),
            dma((8,)),
            dma((7,)),
            dma((5,)),
            dma((5,)),
            dma((3,)),
            dma((3,)),
            dma((1,)),
            dma((1,)),
            dma((3 * HALF_ROW,)),
            dma((3 * HALF_ROW,)),
        ],
        compiler_params=pltpu.CompilerParams(
            collective_id=0, has_side_effects=True, vmem_limit_bytes=54 * 1024 * 1024
        ),
    )(
        x, marks, select, column, norm_gain1, norm_gain2,
        qkv_weight, proj_weight, up_weight, down_weight,
    )
    out = pl.pallas_call(
        settle,
        out_shape=jax.ShapeDtypeStruct(x.shape, BF16),
        in_specs=[vmem],
        out_specs=hbm,
        scratch_shapes=[dma((8,))],
        compiler_params=pltpu.CompilerParams(vmem_limit_bytes=2 * 1024 * 1024),
    )(out)
    return jnp.transpose(out, (2, 0, 1, 3)).reshape(tokens.shape)


def solution(mesh):
    return jax.shard_map(
        per_device,
        mesh=mesh,
        in_specs=(P(None, "lat", "lon", None), P(None, "lat", "lon"), P(), P(), P(), P(), P(), P()),
        out_specs=P(None, "lat", "lon", None),
        check_vma=False,
    )
```

```python
import jax
import jax.numpy as jnp
import numpy as np
from jax import lax
from jax.experimental import pallas as pl
from jax.experimental.pallas import tpu as pltpu
from jax.sharding import PartitionSpec as P

HEADS = 8
WLEV = 2
WLAT = 6
WLON = 12
EPSILON = 1e-05
FAR = -1e30
LANES = 128
MESH = pl.DeviceIdType.MESH
F32 = jnp.float32
BF16 = jnp.bfloat16


def normed(field, gain):
    mean = jnp.mean(field, axis=-1, keepdims=True)
    centered = field - mean
    variance = jnp.mean(centered * centered, axis=-1, keepdims=True)
    return (centered * lax.rsqrt(variance + EPSILON) * gain).astype(BF16)


def gelu(x):
    inner = x * (0.7978845608028654 + 0.035677408136300125 * (x * x))
    half = 0.5 * x
    return half + half * jnp.tanh(inner)


def dot(a, b):
    return jnp.dot(a, b, preferred_element_type=F32)


def dot_t(a, b):
    return lax.dot_general(a, b, (((1,), (1,)), ((), ())), preferred_element_type=F32)


HALF_ROW, HALF_COLUMN = WLAT // 2, WLON // 2
CELL = HALF_ROW * HALF_COLUMN
QUARTER = WLEV * CELL
SPOT = 16


def label_tables(levels):
    windows = levels // WLEV
    select = np.zeros((2, windows * 4 * QUARTER, LANES), np.float32)
    column = np.zeros((windows * 4 * QUARTER, LANES), np.float32)
    rows = 4 * HALF_ROW * levels
    for block in range(2):
        for token in range(select.shape[1]):
            group, rest = divmod(token, 4 * QUARTER)
            place, rest = divmod(rest, QUARTER)
            spot, level = divmod(rest, WLEV)
            row, col = divmod(spot, HALF_COLUMN)
            level = (group * WLEV + level + block * (WLEV // 2)) % levels
            select[block, token, (place * HALF_ROW + row) * levels + level] = 1
            column[token, col + HALF_COLUMN * (place // 2)] = 1
            column[token, SPOT] = 1
            if block == 1:
                select[block, token, rows] = level < WLEV // 2
                select[block, token, rows + 1] = place in (1, 2)
    return jnp.asarray(select, BF16), jnp.asarray(column, F32)


def kernel(
    x_hbm, e_hbm, select_hbm, column_hbm, g1_hbm, g2_hbm,
    wqkv_hbm, wproj_hbm, wup_hbm, wdown_hbm, out_ref,
    xin, region, select, column, g1, g2, regions, own, shift, side, corner, below,
    xs, qkv, heads, marks_q, marks_k, inner, flat, cross, wide, ready, o_send, o_back,
    wqkv, wproj, wup, wdown, wsem, isem, fsend, frecv, esend, erecv, osend, orecv, bsend, brecv,
):
    lat_count, lon_count = lax.axis_size("lat"), lax.axis_size("lon")
    lat, lon = lax.axis_index("lat"), lax.axis_index("lon")
    up = lax.rem(lat + lat_count - 1, lat_count)
    down = lax.rem(lat + 1, lat_count)
    left = lax.rem(lon + lon_count - 1, lon_count)
    right = lax.rem(lon + 1, lon_count)
    before = {"left": (lat, left), "up": (up, lon), "corner": (up, left)}
    after = {"left": (lat, right), "up": (down, lon), "corner": (down, right)}

    spots, lane_tiles, levels, lanes = xin.shape
    features = lane_tiles * lanes
    span = xs.shape[1]
    group = span // 2
    half = group // 2
    hidden = wup.shape[2]
    step = 256
    columns = 2 * HALF_COLUMN
    window_spots = spots // 2

    weights = [
        pltpu.make_async_copy(source.at[block], target.at[block], wsem.at[block * 4 + at])
        for block in range(2)
        for at, (source, target) in enumerate(
            ((wqkv_hbm, wqkv), (wproj_hbm, wproj), (wup_hbm, wup), (wdown_hbm, wdown))
        )
    ]
    halves = [pl.ds(u * window_spots, window_spots) for u in range(2)]
    inputs = [
        pltpu.make_async_copy(source, target, isem.at[at])
        for at, (source, target) in enumerate(
            (
                (x_hbm.at[halves[0]], xin.at[halves[0]]),
                (x_hbm.at[halves[1]], xin.at[halves[1]]),
                (e_hbm, region),
                (select_hbm, select),
                (column_hbm, column),
                (g1_hbm, g1),
                (g2_hbm, g2),
            )
        )
    ]
    inputs[0].start()
    for at in (5, 2, 3, 4):
        inputs[at].start()
    weights[0].start()

    barrier = pltpu.get_barrier_semaphore()
    for device in list(before.values()) + list(after.values()):
        pl.semaphore_signal(barrier, inc=1, device_id=device, device_id_type=MESH)

    moves = (
        (2, 0, 0, "left"),
        (0, 1, 1, "corner"),
        (4, 0, 1, "left"),
        (6, 1, 0, "left"),
        (1, 1, 2, "up"),
    )
    local = {(0, 2): 3, (0, 3): 5, (1, 3): 7}
    arrivals = {(move[1], move[2]): at for at, move in enumerate(moves)}
    returns = ((6, 0, "left"), (0, 1, "corner"), (1, 2, "up"))

    def remote(source, target, send, recv, device):
        return pltpu.make_async_remote_copy(
            source, target, send, recv, device_id=device, device_id_type=MESH
        )

    labels = [
        remote(region.at[HALF_ROW:], side, esend.at[0], erecv.at[0], before["left"]),
        remote(region.at[:HALF_ROW], corner, esend.at[1], erecv.at[1], before["corner"]),
        remote(region.at[:HALF_ROW], below, esend.at[2], erecv.at[2], before["up"]),
    ]
    forward = [
        remote(own.at[atom], shift.at[window, place], fsend.at[at], frecv.at[at], before[towards])
        for at, (atom, window, place, towards) in enumerate(moves)
    ]
    outward = remote(o_send, o_back, osend.at[0], orecv.at[0], after["left"])

    def first_spot(atom, row):
        return ((atom // 2) * HALF_ROW + row) * columns + (atom % 2) * HALF_COLUMN

    backward = [
        remote(
            ready.at[at, pl.ds(row * HALF_COLUMN, HALF_COLUMN)],
            out_ref.at[pl.ds(first_spot(atom, row), HALF_COLUMN)],
            bsend.at[at * HALF_ROW + row],
            brecv.at[at * HALF_ROW + row],
            after[towards],
        )
        for at, (atom, place, towards) in enumerate(returns)
        for row in range(HALF_ROW)
    ]

    lane = lax.broadcasted_iota(jnp.int32, (1, lanes), 1)
    lane_value = lane.astype(F32)
    low = lane < 64
    scale = 64 ** -0.5
    head_masks = (
        jnp.where(low, scale, 0.0).astype(BF16),
        jnp.where(low, 0.0, scale).astype(BF16),
    )

    def tile(at):
        return slice(at * lanes, (at + 1) * lanes)

    def mark(block, at, places):
        index = 2 * block + at
        count = HALF_ROW * levels
        regions[index] = jnp.zeros(regions.shape[1:], F32)
        for place, (source, row) in enumerate(places):
            for r in range(HALF_ROW):
                start = place * count + r * levels
                regions[index, start : start + levels, :columns] = source[row + r].astype(F32)
        if block == 1:
            wrapped = jnp.where(lat == lat_count - 1, 8.0, 0.0) if at == 1 else 0.0
            regions[index, 4 * count : 4 * count + 1, :] = jnp.where(lane == SPOT, 4.0, 0.0)
            regions[index, 4 * count + 1 : 4 * count + 2, :] = jnp.where(lane == SPOT, wrapped, 0.0)
        value = dot(select[block], regions[index].astype(BF16)) * column[...]
        same = jnp.sum(value, axis=-1, keepdims=True) == lane_value
        marks_q[index] = jnp.where(same, FAR, 0.0).astype(BF16)
        marks_k[index] = jnp.where(same, 0.0, 1.0).astype(BF16)

    def project(block, at, spans, first=False):
        index = 2 * block + at
        rows = jnp.concatenate([xs[index, span_at, :] for span_at in spans], axis=0)
        n1 = normed(rows, g1[block : block + 1, :])
        if first:
            weights[block * 4].wait()
        if first and block == 0:
            inputs[1].start()
            inputs[6].start()
            for later in (1, 2, 3):
                weights[later].start()
        mixed = dot(n1, wqkv[block]).astype(BF16)
        start = 0
        for span_at in spans:
            size = span_at.stop - span_at.start
            qkv[index, span_at, :] = mixed[start : start + size]
            start += size

    whole = (slice(0, span),)
    near = (slice(half, group), slice(group + half, span))
    far = (slice(0, half), slice(group, group + half))

    cut = -(-half // 16) * 16

    def attend(block, at, first=0, last=0):
        index = 2 * block + at
        last = last or group
        size = last - first
        ones = jnp.ones((group, lanes), BF16)
        jobs = [(start, at_tile) for start in (0, group) for at_tile in range(lane_tiles)]
        scored, weighted = {}, {}

        def score(start, at_tile):
            rows = slice(start, start + group)
            asked = slice(start + first, start + last)
            mark_q = marks_q[index, asked, :]
            query = qkv[index, asked, tile(at_tile)]
            query = jnp.concatenate([query * head_masks[0], query * head_masks[1]], axis=0)
            key = qkv[index, rows, tile(lane_tiles + at_tile)]
            return dot_t(
                jnp.concatenate([query, jnp.concatenate([mark_q, mark_q], axis=0)], axis=1),
                jnp.concatenate([key, marks_k[index, rows, :]], axis=1),
            )

        def weigh(scores):
            peak = jnp.max(scores, axis=-1, keepdims=True)
            return jnp.exp(scores - peak).astype(BF16)

        def mix(start, at_tile, weight):
            rows = slice(start, start + group)
            value = qkv[index, rows, tile(2 * lane_tiles + at_tile)]
            total = dot(weight, jnp.concatenate([value, ones], axis=1))
            over = jnp.where(low, total[:size, :lanes], total[size:, :lanes])
            under = jnp.where(low, total[:size, lanes:], total[size:, lanes:])
            asked = slice(start + first, start + last)
            heads[index, asked, tile(at_tile)] = over / under

        for at_job in range(len(jobs) + 2):
            if at_job < len(jobs):
                scored[at_job] = score(*jobs[at_job])
            if 0 <= at_job - 1 < len(jobs):
                weighted[at_job - 1] = weigh(scored.pop(at_job - 1))
            if at_job >= 2:
                mix(*jobs[at_job - 2], weighted.pop(at_job - 2))

    def gather(source, parts):
        pieces = []
        for index, which in parts:
            for start in (which * half, group + which * half):
                pieces.append(source[index, start : start + half, :])
        return jnp.concatenate(pieces, axis=0)

    def mlp(block, h, mixed, first=False):
        if first:
            weights[block * 4 + 1].wait()
        h = h + dot(mixed, wproj[block])
        n2 = normed(h, g2[block : block + 1, :])
        if first:
            weights[block * 4 + 2].wait()
        count = h.shape[0]
        for at in range(0, hidden, step):
            inner[:count, at : at + step] = gelu(
                dot(n2, wup[block, :, at : at + step]).astype(BF16)
            )
        if first:
            weights[block * 4 + 3].wait()
        return h + dot(inner[:count, :], wdown[block])

    def relevel(slot, h, shifts, targets, stride):
        for at in range(lane_tiles):
            flat[slot, at] = h[:, tile(at)]
        for place, target in enumerate(targets):
            for at in range(lane_tiles):
                for group_at in range(2):
                    for lev in range(WLEV):
                        source = group_at * half + place * QUARTER + lev
                        target[at, pl.ds(shifts[group_at][lev], CELL, stride=stride)] = flat[
                            slot, at, pl.ds(source, CELL, stride=WLEV)
                        ]

    def finish_first(slot, h, atoms):
        targets = [cross.at[slot, place] for place in range(2)]
        relevel(slot, h, ((QUARTER + 1, 0), (1, QUARTER)), targets, WLEV)
        for place, atom in enumerate(atoms):
            for at in range(lane_tiles):
                own[atom, :, tile(at)] = cross[slot, place, at].astype(BF16)

    def finish_second(slot, h, results):
        targets = [wide.at[slot, place] for place in range(2)]
        relevel(slot, h, ((1, 2), (3, 0)), targets, levels)
        for place, result in enumerate(results):
            for spot in range(CELL):
                row, col = divmod(spot, HALF_COLUMN)
                for at in range(lane_tiles):
                    value = wide[slot, place, at, spot * levels : (spot + 1) * levels].astype(BF16)
                    if result[0] == "out":
                        out_ref[first_spot(result[1], row) + col, at] = value
                    else:
                        ready[result[1], spot, at] = value
            if result[0] == "send":
                for row in range(HALF_ROW):
                    backward[result[1] * HALF_ROW + row].start()

    def load_first(u):
        if u:
            inputs[u].wait()
        for spot in range(window_spots):
            row, col = divmod(spot, columns)
            place = (col // HALF_COLUMN) * 2 + row // HALF_ROW
            at_spot = (row % HALF_ROW) * HALF_COLUMN + col % HALF_COLUMN
            start = place * QUARTER + at_spot * WLEV
            for at in range(lane_tiles):
                value = xin[u * window_spots + spot, at].astype(F32)
                for group_at in range(2):
                    xs[u, group_at * group + start : group_at * group + start + WLEV, tile(at)] = (
                        value[group_at * WLEV : (group_at + 1) * WLEV]
                    )

    def own_regions(u):
        places = [(region, u * WLAT), (region, u * WLAT + HALF_ROW)]
        return places + places

    def load_second(w, places):
        for place in places:
            if (w, place) in arrivals:
                forward[arrivals[w, place]].wait_recv()
                value = shift[w, place].astype(F32)
            else:
                value = own[local[w, place]].astype(F32)
            for group_at in range(2):
                start = group_at * group + place * QUARTER
                xs[2 + w, start : start + QUARTER, :] = value[
                    group_at * QUARTER : (group_at + 1) * QUARTER
                ]

    inputs[0].wait()
    load_first(0)
    inputs[2].wait()
    inputs[3].wait()
    inputs[4].wait()
    mark(0, 0, own_regions(0))
    inputs[5].wait()
    project(0, 0, whole, True)
    pl.semaphore_wait(barrier, 6)
    for copy in labels:
        copy.start()
    attend(0, 0, 0, cut)
    inputs[6].wait()
    h = mlp(0, gather(xs, [(0, 0)]), gather(heads, [(0, 0)]).astype(BF16), True)
    finish_first(0, h, (0, 2))
    forward[0].start()
    forward[1].start()
    for at in range(4, 8):
        weights[at].start()
    load_first(1)
    mark(0, 1, own_regions(1))
    project(0, 1, whole)
    attend(0, 1, 0, cut)
    h = mlp(0, gather(xs, [(1, 0)]), gather(heads, [(1, 0)]).astype(BF16))
    finish_first(1, h, (4, 6))
    forward[2].start()
    forward[3].start()
    attend(0, 0, cut, group)
    attend(0, 1, cut, group)
    parts = [(0, 1), (1, 1)]
    h = mlp(0, gather(xs, parts), gather(heads, parts).astype(BF16))
    finish_first(0, h[:group], (1, 3))
    forward[4].start()
    finish_first(1, h[group:], (5, 7))

    for copy in labels:
        copy.wait_recv()
    load_second(0, (2, 3))
    project(1, 0, near, True)
    mark(1, 0, [(side, 0), (side, HALF_ROW), (region, HALF_ROW), (region, 2 * HALF_ROW)])
    mark(1, 1, [(side, 2 * HALF_ROW), (corner, 0), (below, 0), (region, 3 * HALF_ROW)])
    load_second(0, (0, 1))
    project(1, 0, far)
    attend(1, 0)
    o_send[...] = gather(heads, [(2, 0)]).astype(BF16)
    outward.start()
    load_second(1, (0, 1, 2, 3))
    project(1, 1, whole)
    attend(1, 1)
    h = mlp(1, gather(xs, [(3, 0)]), gather(heads, [(3, 0)]).astype(BF16), True)
    finish_second(0, h, (("send", 0), ("send", 1)))
    parts = [(3, 1), (2, 1)]
    h = mlp(1, gather(xs, parts), gather(heads, parts).astype(BF16))
    finish_second(1, h[:group], (("send", 2), ("out", 7)))
    finish_second(0, h[group:], (("out", 3), ("out", 5)))
    pieces = [own[2].astype(F32), own[4].astype(F32)]
    residual = jnp.concatenate(
        [piece[:QUARTER] for piece in pieces] + [piece[QUARTER:] for piece in pieces], axis=0
    )
    outward.wait_recv()
    h = mlp(1, residual, o_back[...])
    finish_second(1, h, (("out", 2), ("out", 4)))
    for copy in backward:
        copy.wait_recv()
    for copy in labels + forward + [outward] + backward:
        copy.wait_send()


def settle(source, target, sems):
    chunks = sems.shape[0]
    size = source.shape[0] // chunks
    copies = [
        pltpu.make_async_copy(
            source.at[pl.ds(at * size, size)], target.at[pl.ds(at * size, size)], sems.at[at]
        )
        for at in range(chunks)
    ]
    for copy in copies:
        copy.start()
    for copy in copies:
        copy.wait()


def per_device(
    tokens, region, norm_gain1, qkv_weight, proj_weight, norm_gain2, up_weight, down_weight
):
    levels, row_count, column_count, features = tokens.shape
    hidden = up_weight.shape[2]
    lane_tiles = features // LANES
    spots = row_count * column_count
    quarter_rows = levels * CELL
    span = 4 * quarter_rows
    group = span // 2
    x = jnp.transpose(tokens.reshape(levels, spots, lane_tiles, LANES), (1, 2, 0, 3))
    marks = jnp.transpose(region, (1, 0, 2))
    select, column = label_tables(levels)

    vmem = pl.BlockSpec(memory_space=pltpu.VMEM)
    hbm = pl.BlockSpec(memory_space=pl.ANY)
    dma = pltpu.SemaphoreType.DMA
    out = pl.pallas_call(
        kernel,
        out_shape=pltpu.VMEM(x.shape, BF16),
        in_specs=[hbm] * 10,
        out_specs=vmem,
        scratch_shapes=[
            pltpu.VMEM(x.shape, BF16),
            pltpu.VMEM(marks.shape, jnp.int32),
            pltpu.VMEM(select.shape, BF16),
            pltpu.VMEM(column.shape, F32),
            pltpu.VMEM(norm_gain1.shape, F32),
            pltpu.VMEM(norm_gain2.shape, F32),
            pltpu.VMEM((4, LANES, LANES), F32),
            pltpu.VMEM((8, quarter_rows, features), BF16),
            pltpu.VMEM((2, 4, quarter_rows, features), BF16),
            pltpu.VMEM((row_count - HALF_ROW,) + marks.shape[1:], jnp.int32),
            pltpu.VMEM((HALF_ROW,) + marks.shape[1:], jnp.int32),
            pltpu.VMEM((HALF_ROW,) + marks.shape[1:], jnp.int32),
            pltpu.VMEM((4, span, features), F32),
            pltpu.VMEM((4, span, 3 * features), BF16),
            pltpu.VMEM((4, span, features), F32),
            pltpu.VMEM((4, span, LANES), BF16),
            pltpu.VMEM((4, span, LANES), BF16),
            pltpu.VMEM((span, hidden), BF16),
            pltpu.VMEM((2, lane_tiles, group, LANES), F32),
            pltpu.VMEM((2, 2, lane_tiles, quarter_rows, LANES), F32),
            pltpu.VMEM((2, 2, lane_tiles, quarter_rows, LANES), F32),
            pltpu.VMEM((3, CELL) + x.shape[1:], BF16),
            pltpu.VMEM((group, features), BF16),
            pltpu.VMEM((group, features), BF16),
            pltpu.VMEM(qkv_weight.shape, BF16),
            pltpu.VMEM(proj_weight.shape, BF16),
            pltpu.VMEM(up_weight.shape, BF16),
            pltpu.VMEM(down_weight.shape, BF16),
            dma((8,)),
            dma((7,)),
            dma((5,)),
            dma((5,)),
            dma((3,)),
            dma((3,)),
            dma((1,)),
            dma((1,)),
            dma((3 * HALF_ROW,)),
            dma((3 * HALF_ROW,)),
        ],
        compiler_params=pltpu.CompilerParams(
            collective_id=0, has_side_effects=True, vmem_limit_bytes=54 * 1024 * 1024
        ),
    )(
        x, marks, select, column, norm_gain1, norm_gain2,
        qkv_weight, proj_weight, up_weight, down_weight,
    )
    out = pl.pallas_call(
        settle,
        out_shape=jax.ShapeDtypeStruct(x.shape, BF16),
        in_specs=[vmem],
        out_specs=hbm,
        scratch_shapes=[dma((8,))],
        compiler_params=pltpu.CompilerParams(vmem_limit_bytes=2 * 1024 * 1024),
    )(out)
    return jnp.transpose(out, (2, 0, 1, 3)).reshape(tokens.shape)


def solution(mesh):
    return jax.shard_map(
        per_device,
        mesh=mesh,
        in_specs=(P(None, "lat", "lon", None), P(None, "lat", "lon"), P(), P(), P(), P(), P(), P()),
        out_specs=P(None, "lat", "lon", None),
        check_vma=False,
    )
```

```python
import jax
import jax.numpy as jnp
import numpy as np
from jax import lax
from jax.experimental import pallas as pl
from jax.experimental.pallas import tpu as pltpu
from jax.sharding import PartitionSpec as P

HEADS = 8
WLEV = 2
WLAT = 6
WLON = 12
EPSILON = 1e-05
FAR = -1e30
LANES = 128
MESH = pl.DeviceIdType.MESH
F32 = jnp.float32
BF16 = jnp.bfloat16


def normed(field, gain):
    mean = jnp.mean(field, axis=-1, keepdims=True)
    centered = field - mean
    variance = jnp.mean(centered * centered, axis=-1, keepdims=True)
    return (centered * lax.rsqrt(variance + EPSILON) * gain).astype(BF16)


def gelu(x):
    inner = x * (0.7978845608028654 + 0.035677408136300125 * (x * x))
    half = 0.5 * x
    return half + half * jnp.tanh(inner)


def dot(a, b):
    return jnp.dot(a, b, preferred_element_type=F32)


def dot_t(a, b):
    return lax.dot_general(a, b, (((1,), (1,)), ((), ())), preferred_element_type=F32)


HALF_ROW, HALF_COLUMN = WLAT // 2, WLON // 2
CELL = HALF_ROW * HALF_COLUMN
QUARTER = WLEV * CELL
SPOT = 16


def label_tables(levels):
    windows = levels // WLEV
    select = np.zeros((2, windows * 4 * QUARTER, LANES), np.float32)
    column = np.zeros((windows * 4 * QUARTER, LANES), np.float32)
    rows = 4 * HALF_ROW * levels
    for block in range(2):
        for token in range(select.shape[1]):
            group, rest = divmod(token, 4 * QUARTER)
            place, rest = divmod(rest, QUARTER)
            spot, level = divmod(rest, WLEV)
            row, col = divmod(spot, HALF_COLUMN)
            level = (group * WLEV + level + block * (WLEV // 2)) % levels
            select[block, token, (place * HALF_ROW + row) * levels + level] = 1
            column[token, col + HALF_COLUMN * (place // 2)] = 1
            column[token, SPOT] = 1
            if block == 1:
                select[block, token, rows] = level < WLEV // 2
                select[block, token, rows + 1] = place in (1, 2)
    return jnp.asarray(select, BF16), jnp.asarray(column, F32)


def kernel(
    x_hbm, e_hbm, select_hbm, column_hbm, g1_hbm, g2_hbm,
    wqkv_hbm, wproj_hbm, wup_hbm, wdown_hbm, out_ref,
    xin, region, select, column, g1, g2, regions, own, shift, side, corner, below,
    xs, qkv, heads, marks_q, marks_k, inner, flat, cross, wide, ready, o_send, o_back,
    wqkv, wproj, wup, wdown, wsem, isem, fsend, frecv, esend, erecv, osend, orecv, bsend, brecv,
):
    lat_count, lon_count = lax.axis_size("lat"), lax.axis_size("lon")
    lat, lon = lax.axis_index("lat"), lax.axis_index("lon")
    up = lax.rem(lat + lat_count - 1, lat_count)
    down = lax.rem(lat + 1, lat_count)
    left = lax.rem(lon + lon_count - 1, lon_count)
    right = lax.rem(lon + 1, lon_count)
    before = {"left": (lat, left), "up": (up, lon), "corner": (up, left)}
    after = {"left": (lat, right), "up": (down, lon), "corner": (down, right)}

    spots, lane_tiles, levels, lanes = xin.shape
    features = lane_tiles * lanes
    span = xs.shape[1]
    group = span // 2
    half = group // 2
    hidden = wup.shape[2]
    step = 256
    columns = 2 * HALF_COLUMN
    window_spots = spots // 2

    weights = [
        pltpu.make_async_copy(source.at[block], target.at[block], wsem.at[block * 4 + at])
        for block in range(2)
        for at, (source, target) in enumerate(
            ((wqkv_hbm, wqkv), (wproj_hbm, wproj), (wup_hbm, wup), (wdown_hbm, wdown))
        )
    ]
    halves = [pl.ds(u * window_spots, window_spots) for u in range(2)]
    inputs = [
        pltpu.make_async_copy(source, target, isem.at[at])
        for at, (source, target) in enumerate(
            (
                (x_hbm.at[halves[0]], xin.at[halves[0]]),
                (x_hbm.at[halves[1]], xin.at[halves[1]]),
                (e_hbm, region),
                (select_hbm, select),
                (column_hbm, column),
                (g1_hbm, g1),
                (g2_hbm, g2),
            )
        )
    ]
    inputs[0].start()
    for at in (5, 2, 3, 4):
        inputs[at].start()
    weights[0].start()

    barrier = pltpu.get_barrier_semaphore()
    for device in list(before.values()) + list(after.values()):
        pl.semaphore_signal(barrier, inc=1, device_id=device, device_id_type=MESH)

    moves = (
        (2, 0, 0, "left"),
        (0, 1, 1, "corner"),
        (4, 0, 1, "left"),
        (6, 1, 0, "left"),
        (1, 1, 2, "up"),
    )
    local = {(0, 2): 3, (0, 3): 5, (1, 3): 7}
    arrivals = {(move[1], move[2]): at for at, move in enumerate(moves)}
    returns = ((6, 0, "left"), (0, 1, "corner"), (1, 2, "up"))

    def remote(source, target, send, recv, device):
        return pltpu.make_async_remote_copy(
            source, target, send, recv, device_id=device, device_id_type=MESH
        )

    labels = [
        remote(region.at[HALF_ROW:], side, esend.at[0], erecv.at[0], before["left"]),
        remote(region.at[:HALF_ROW], corner, esend.at[1], erecv.at[1], before["corner"]),
        remote(region.at[:HALF_ROW], below, esend.at[2], erecv.at[2], before["up"]),
    ]
    forward = [
        remote(own.at[atom], shift.at[window, place], fsend.at[at], frecv.at[at], before[towards])
        for at, (atom, window, place, towards) in enumerate(moves)
    ]
    outward = remote(o_send, o_back, osend.at[0], orecv.at[0], after["left"])

    def first_spot(atom, row):
        return ((atom // 2) * HALF_ROW + row) * columns + (atom % 2) * HALF_COLUMN

    backward = [
        remote(
            ready.at[at, pl.ds(row * HALF_COLUMN, HALF_COLUMN)],
            out_ref.at[pl.ds(first_spot(atom, row), HALF_COLUMN)],
            bsend.at[at * HALF_ROW + row],
            brecv.at[at * HALF_ROW + row],
            after[towards],
        )
        for at, (atom, place, towards) in enumerate(returns)
        for row in range(HALF_ROW)
    ]

    lane = lax.broadcasted_iota(jnp.int32, (1, lanes), 1)
    lane_value = lane.astype(F32)
    low = lane < 64
    scale = 64 ** -0.5
    head_masks = (
        jnp.where(low, scale, 0.0).astype(BF16),
        jnp.where(low, 0.0, scale).astype(BF16),
    )

    def tile(at):
        return slice(at * lanes, (at + 1) * lanes)

    def mark(block, at, places):
        index = 2 * block + at
        count = HALF_ROW * levels
        regions[index] = jnp.zeros(regions.shape[1:], F32)
        for place, (source, row) in enumerate(places):
            for r in range(HALF_ROW):
                start = place * count + r * levels
                regions[index, start : start + levels, :columns] = source[row + r].astype(F32)
        if block == 1:
            wrapped = jnp.where(lat == lat_count - 1, 8.0, 0.0) if at == 1 else 0.0
            regions[index, 4 * count : 4 * count + 1, :] = jnp.where(lane == SPOT, 4.0, 0.0)
            regions[index, 4 * count + 1 : 4 * count + 2, :] = jnp.where(lane == SPOT, wrapped, 0.0)
        value = dot(select[block], regions[index].astype(BF16)) * column[...]
        same = jnp.sum(value, axis=-1, keepdims=True) == lane_value
        marks_q[index] = jnp.where(same, FAR, 0.0).astype(BF16)
        marks_k[index] = jnp.where(same, 0.0, 1.0).astype(BF16)

    def project(block, at, spans, first=False):
        index = 2 * block + at
        rows = jnp.concatenate([xs[index, span_at, :] for span_at in spans], axis=0)
        n1 = normed(rows, g1[block : block + 1, :])
        if first:
            weights[block * 4].wait()
        if first and block == 0:
            inputs[1].start()
            inputs[6].start()
            for later in (1, 2, 3):
                weights[later].start()
        mixed = dot(n1, wqkv[block]).astype(BF16)
        start = 0
        for span_at in spans:
            size = span_at.stop - span_at.start
            qkv[index, span_at, :] = mixed[start : start + size]
            start += size

    whole = (slice(0, span),)
    near = (slice(half, group), slice(group + half, span))
    far = (slice(0, half), slice(group, group + half))

    cut = -(-half // 16) * 16

    def attend(block, at, first=0, last=0):
        index = 2 * block + at
        last = last or group
        size = last - first
        ones = jnp.ones((group, lanes), BF16)
        jobs = [(start, at_tile) for start in (0, group) for at_tile in range(lane_tiles)]
        scored, weighted = {}, {}

        def score(start, at_tile):
            rows = slice(start, start + group)
            asked = slice(start + first, start + last)
            mark_q = marks_q[index, asked, :]
            query = qkv[index, asked, tile(at_tile)]
            query = jnp.concatenate([query * head_masks[0], query * head_masks[1]], axis=0)
            key = qkv[index, rows, tile(lane_tiles + at_tile)]
            return dot_t(
                jnp.concatenate([query, jnp.concatenate([mark_q, mark_q], axis=0)], axis=1),
                jnp.concatenate([key, marks_k[index, rows, :]], axis=1),
            )

        def weigh(scores):
            peak = jnp.max(scores, axis=-1, keepdims=True)
            return jnp.exp(scores - peak).astype(BF16)

        def mix(start, at_tile, weight):
            rows = slice(start, start + group)
            value = qkv[index, rows, tile(2 * lane_tiles + at_tile)]
            total = dot(weight, jnp.concatenate([value, ones], axis=1))
            over = jnp.where(low, total[:size, :lanes], total[size:, :lanes])
            under = jnp.where(low, total[:size, lanes:], total[size:, lanes:])
            asked = slice(start + first, start + last)
            heads[index, asked, tile(at_tile)] = over / under

        for at_job in range(len(jobs) + 2):
            if at_job < len(jobs):
                scored[at_job] = score(*jobs[at_job])
            if 0 <= at_job - 1 < len(jobs):
                weighted[at_job - 1] = weigh(scored.pop(at_job - 1))
            if at_job >= 2:
                mix(*jobs[at_job - 2], weighted.pop(at_job - 2))

    def gather(source, parts):
        pieces = []
        for index, which in parts:
            for start in (which * half, group + which * half):
                pieces.append(source[index, start : start + half, :])
        return jnp.concatenate(pieces, axis=0)

    def mlp(block, h, mixed, first=False):
        if first:
            weights[block * 4 + 1].wait()
        h = h + dot(mixed, wproj[block])
        n2 = normed(h, g2[block : block + 1, :])
        if first:
            weights[block * 4 + 2].wait()
        count = h.shape[0]
        for at in range(0, hidden, step):
            inner[:count, at : at + step] = gelu(
                dot(n2, wup[block, :, at : at + step]).astype(BF16)
            )
        if first:
            weights[block * 4 + 3].wait()
        return h + dot(inner[:count, :], wdown[block])

    def relevel(slot, h, shifts, targets, stride):
        for at in range(lane_tiles):
            flat[slot, at] = h[:, tile(at)]
        for place, target in enumerate(targets):
            for at in range(lane_tiles):
                for group_at in range(2):
                    for lev in range(WLEV):
                        source = group_at * half + place * QUARTER + lev
                        target[at, pl.ds(shifts[group_at][lev], CELL, stride=stride)] = flat[
                            slot, at, pl.ds(source, CELL, stride=WLEV)
                        ]

    def finish_first(slot, h, atoms):
        targets = [cross.at[slot, place] for place in range(2)]
        relevel(slot, h, ((QUARTER + 1, 0), (1, QUARTER)), targets, WLEV)
        for place, atom in enumerate(atoms):
            for at in range(lane_tiles):
                own[atom, :, tile(at)] = cross[slot, place, at].astype(BF16)

    def finish_second(slot, h, results):
        targets = [wide.at[slot, place] for place in range(2)]
        relevel(slot, h, ((1, 2), (3, 0)), targets, levels)
        for place, result in enumerate(results):
            for spot in range(CELL):
                row, col = divmod(spot, HALF_COLUMN)
                for at in range(lane_tiles):
                    value = wide[slot, place, at, spot * levels : (spot + 1) * levels].astype(BF16)
                    if result[0] == "out":
                        out_ref[first_spot(result[1], row) + col, at] = value
                    else:
                        ready[result[1], spot, at] = value
            if result[0] == "send":
                for row in range(HALF_ROW):
                    backward[result[1] * HALF_ROW + row].start()

    def load_first(u):
        if u:
            inputs[u].wait()
        for spot in range(window_spots):
            row, col = divmod(spot, columns)
            place = (col // HALF_COLUMN) * 2 + row // HALF_ROW
            at_spot = (row % HALF_ROW) * HALF_COLUMN + col % HALF_COLUMN
            start = place * QUARTER + at_spot * WLEV
            for at in range(lane_tiles):
                value = xin[u * window_spots + spot, at].astype(F32)
                for group_at in range(2):
                    xs[u, group_at * group + start : group_at * group + start + WLEV, tile(at)] = (
                        value[group_at * WLEV : (group_at + 1) * WLEV]
                    )

    def own_regions(u):
        places = [(region, u * WLAT), (region, u * WLAT + HALF_ROW)]
        return places + places

    def load_second(w, places):
        for place in places:
            if (w, place) in arrivals:
                forward[arrivals[w, place]].wait_recv()
                value = shift[w, place].astype(F32)
            else:
                value = own[local[w, place]].astype(F32)
            for group_at in range(2):
                start = group_at * group + place * QUARTER
                xs[2 + w, start : start + QUARTER, :] = value[
                    group_at * QUARTER : (group_at + 1) * QUARTER
                ]

    inputs[0].wait()
    load_first(0)
    inputs[2].wait()
    inputs[3].wait()
    inputs[4].wait()
    mark(0, 0, own_regions(0))
    inputs[5].wait()
    project(0, 0, whole, True)
    pl.semaphore_wait(barrier, 6)
    for copy in labels:
        copy.start()
    attend(0, 0, 0, cut)
    inputs[6].wait()
    h = mlp(0, gather(xs, [(0, 0)]), gather(heads, [(0, 0)]).astype(BF16), True)
    finish_first(0, h, (0, 2))
    forward[0].start()
    forward[1].start()
    for at in range(4, 8):
        weights[at].start()
    load_first(1)
    mark(0, 1, own_regions(1))
    project(0, 1, whole)
    attend(0, 1, 0, cut)
    h = mlp(0, gather(xs, [(1, 0)]), gather(heads, [(1, 0)]).astype(BF16))
    finish_first(1, h, (4, 6))
    forward[2].start()
    forward[3].start()
    attend(0, 0, cut, group)
    attend(0, 1, cut, group)
    parts = [(0, 1), (1, 1)]
    h = mlp(0, gather(xs, parts), gather(heads, parts).astype(BF16))
    finish_first(0, h[:group], (1, 3))
    forward[4].start()
    finish_first(1, h[group:], (5, 7))

    for copy in labels:
        copy.wait_recv()
    load_second(0, (2, 3))
    project(1, 0, near, True)
    mark(1, 0, [(side, 0), (side, HALF_ROW), (region, HALF_ROW), (region, 2 * HALF_ROW)])
    mark(1, 1, [(side, 2 * HALF_ROW), (corner, 0), (below, 0), (region, 3 * HALF_ROW)])
    load_second(0, (0, 1))
    project(1, 0, far)
    attend(1, 0)
    o_send[...] = gather(heads, [(2, 0)]).astype(BF16)
    outward.start()
    load_second(1, (0, 1, 2, 3))
    project(1, 1, whole)
    attend(1, 1)
    h = mlp(1, gather(xs, [(3, 0)]), gather(heads, [(3, 0)]).astype(BF16), True)
    finish_second(0, h, (("send", 0), ("send", 1)))
    h = mlp(1, gather(xs, [(3, 1)]), gather(heads, [(3, 1)]).astype(BF16))
    finish_second(1, h, (("send", 2), ("out", 7)))
    pieces = [own[2].astype(F32), own[4].astype(F32)]
    residual = [piece[:QUARTER] for piece in pieces] + [piece[QUARTER:] for piece in pieces]
    outward.wait_recv()
    h = mlp(
        1,
        jnp.concatenate([gather(xs, [(2, 1)])] + residual, axis=0),
        jnp.concatenate([gather(heads, [(2, 1)]).astype(BF16), o_back[...]], axis=0),
    )
    finish_second(0, h[:group], (("out", 3), ("out", 5)))
    finish_second(1, h[group:], (("out", 2), ("out", 4)))
    for copy in backward:
        copy.wait_recv()
    for copy in labels + forward + [outward] + backward:
        copy.wait_send()


def settle(source, target, sems):
    chunks = sems.shape[0]
    size = source.shape[0] // chunks
    copies = [
        pltpu.make_async_copy(
            source.at[pl.ds(at * size, size)], target.at[pl.ds(at * size, size)], sems.at[at]
        )
        for at in range(chunks)
    ]
    for copy in copies:
        copy.start()
    for copy in copies:
        copy.wait()


def per_device(
    tokens, region, norm_gain1, qkv_weight, proj_weight, norm_gain2, up_weight, down_weight
):
    levels, row_count, column_count, features = tokens.shape
    hidden = up_weight.shape[2]
    lane_tiles = features // LANES
    spots = row_count * column_count
    quarter_rows = levels * CELL
    span = 4 * quarter_rows
    group = span // 2
    x = jnp.transpose(tokens.reshape(levels, spots, lane_tiles, LANES), (1, 2, 0, 3))
    marks = jnp.transpose(region, (1, 0, 2))
    select, column = label_tables(levels)

    vmem = pl.BlockSpec(memory_space=pltpu.VMEM)
    hbm = pl.BlockSpec(memory_space=pl.ANY)
    dma = pltpu.SemaphoreType.DMA
    out = pl.pallas_call(
        kernel,
        out_shape=pltpu.VMEM(x.shape, BF16),
        in_specs=[hbm] * 10,
        out_specs=vmem,
        scratch_shapes=[
            pltpu.VMEM(x.shape, BF16),
            pltpu.VMEM(marks.shape, jnp.int32),
            pltpu.VMEM(select.shape, BF16),
            pltpu.VMEM(column.shape, F32),
            pltpu.VMEM(norm_gain1.shape, F32),
            pltpu.VMEM(norm_gain2.shape, F32),
            pltpu.VMEM((4, LANES, LANES), F32),
            pltpu.VMEM((8, quarter_rows, features), BF16),
            pltpu.VMEM((2, 4, quarter_rows, features), BF16),
            pltpu.VMEM((row_count - HALF_ROW,) + marks.shape[1:], jnp.int32),
            pltpu.VMEM((HALF_ROW,) + marks.shape[1:], jnp.int32),
            pltpu.VMEM((HALF_ROW,) + marks.shape[1:], jnp.int32),
            pltpu.VMEM((4, span, features), F32),
            pltpu.VMEM((4, span, 3 * features), BF16),
            pltpu.VMEM((4, span, features), F32),
            pltpu.VMEM((4, span, LANES), BF16),
            pltpu.VMEM((4, span, LANES), BF16),
            pltpu.VMEM((span, hidden), BF16),
            pltpu.VMEM((2, lane_tiles, group, LANES), F32),
            pltpu.VMEM((2, 2, lane_tiles, quarter_rows, LANES), F32),
            pltpu.VMEM((2, 2, lane_tiles, quarter_rows, LANES), F32),
            pltpu.VMEM((3, CELL) + x.shape[1:], BF16),
            pltpu.VMEM((group, features), BF16),
            pltpu.VMEM((group, features), BF16),
            pltpu.VMEM(qkv_weight.shape, BF16),
            pltpu.VMEM(proj_weight.shape, BF16),
            pltpu.VMEM(up_weight.shape, BF16),
            pltpu.VMEM(down_weight.shape, BF16),
            dma((8,)),
            dma((7,)),
            dma((5,)),
            dma((5,)),
            dma((3,)),
            dma((3,)),
            dma((1,)),
            dma((1,)),
            dma((3 * HALF_ROW,)),
            dma((3 * HALF_ROW,)),
        ],
        compiler_params=pltpu.CompilerParams(
            collective_id=0, has_side_effects=True, vmem_limit_bytes=54 * 1024 * 1024
        ),
    )(
        x, marks, select, column, norm_gain1, norm_gain2,
        qkv_weight, proj_weight, up_weight, down_weight,
    )
    out = pl.pallas_call(
        settle,
        out_shape=jax.ShapeDtypeStruct(x.shape, BF16),
        in_specs=[vmem],
        out_specs=hbm,
        scratch_shapes=[dma((8,))],
        compiler_params=pltpu.CompilerParams(vmem_limit_bytes=2 * 1024 * 1024),
    )(out)
    return jnp.transpose(out, (2, 0, 1, 3)).reshape(tokens.shape)


def solution(mesh):
    return jax.shard_map(
        per_device,
        mesh=mesh,
        in_specs=(P(None, "lat", "lon", None), P(None, "lat", "lon"), P(), P(), P(), P(), P(), P()),
        out_specs=P(None, "lat", "lon", None),
        check_vma=False,
    )
```

```python
import jax
import jax.numpy as jnp
import numpy as np
from jax import lax
from jax.experimental import pallas as pl
from jax.experimental.pallas import tpu as pltpu
from jax.sharding import PartitionSpec as P

HEADS = 8
WLEV = 2
WLAT = 6
WLON = 12
EPSILON = 1e-05
FAR = -1e30
LANES = 128
MESH = pl.DeviceIdType.MESH
F32 = jnp.float32
BF16 = jnp.bfloat16


def normed(field, gain):
    mean = jnp.mean(field, axis=-1, keepdims=True)
    centered = field - mean
    variance = jnp.mean(centered * centered, axis=-1, keepdims=True)
    return (centered * lax.rsqrt(variance + EPSILON) * gain).astype(BF16)


def gelu(x):
    inner = x * (0.7978845608028654 + 0.035677408136300125 * (x * x))
    half = 0.5 * x
    return half + half * jnp.tanh(inner)


def dot(a, b):
    return jnp.dot(a, b, preferred_element_type=F32)


def dot_t(a, b):
    return lax.dot_general(a, b, (((1,), (1,)), ((), ())), preferred_element_type=F32)


HALF_ROW, HALF_COLUMN = WLAT // 2, WLON // 2
CELL = HALF_ROW * HALF_COLUMN
QUARTER = WLEV * CELL
SPOT = 16


def label_tables(levels):
    windows = levels // WLEV
    select = np.zeros((2, windows * 4 * QUARTER, LANES), np.float32)
    column = np.zeros((windows * 4 * QUARTER, LANES), np.float32)
    rows = 4 * HALF_ROW * levels
    for block in range(2):
        for token in range(select.shape[1]):
            group, rest = divmod(token, 4 * QUARTER)
            place, rest = divmod(rest, QUARTER)
            spot, level = divmod(rest, WLEV)
            row, col = divmod(spot, HALF_COLUMN)
            level = (group * WLEV + level + block * (WLEV // 2)) % levels
            select[block, token, (place * HALF_ROW + row) * levels + level] = 1
            column[token, col + HALF_COLUMN * (place // 2)] = 1
            column[token, SPOT] = 1
            if block == 1:
                select[block, token, rows] = level < WLEV // 2
                select[block, token, rows + 1] = place in (1, 2)
    return jnp.asarray(select, BF16), jnp.asarray(column, F32)


def kernel(
    x_hbm, e_hbm, select_hbm, column_hbm, g1_hbm, g2_hbm,
    wqkv_hbm, wproj_hbm, wup_hbm, wdown_hbm, out_ref,
    xin, region, select, column, g1, g2, regions, own, shift, side, corner, below,
    xs, qkv, heads, marks_q, marks_k, inner, flat, cross, wide, ready, o_send, o_back,
    wqkv, wproj, wup, wdown, wsem, isem, fsend, frecv, esend, erecv, osend, orecv, bsend, brecv,
):
    lat_count, lon_count = lax.axis_size("lat"), lax.axis_size("lon")
    lat, lon = lax.axis_index("lat"), lax.axis_index("lon")
    up = lax.rem(lat + lat_count - 1, lat_count)
    down = lax.rem(lat + 1, lat_count)
    left = lax.rem(lon + lon_count - 1, lon_count)
    right = lax.rem(lon + 1, lon_count)
    before = {"left": (lat, left), "up": (up, lon), "corner": (up, left)}
    after = {"left": (lat, right), "up": (down, lon), "corner": (down, right)}

    spots, lane_tiles, levels, lanes = xin.shape
    features = lane_tiles * lanes
    span = xs.shape[1]
    group = span // 2
    half = group // 2
    hidden = wup.shape[2]
    step = 512
    columns = 2 * HALF_COLUMN
    window_spots = spots // 2

    weights = [
        pltpu.make_async_copy(source.at[block], target.at[block], wsem.at[block * 4 + at])
        for block in range(2)
        for at, (source, target) in enumerate(
            ((wqkv_hbm, wqkv), (wproj_hbm, wproj), (wup_hbm, wup), (wdown_hbm, wdown))
        )
    ]
    halves = [pl.ds(u * window_spots, window_spots) for u in range(2)]
    inputs = [
        pltpu.make_async_copy(source, target, isem.at[at])
        for at, (source, target) in enumerate(
            (
                (x_hbm.at[halves[0]], xin.at[halves[0]]),
                (x_hbm.at[halves[1]], xin.at[halves[1]]),
                (e_hbm, region),
                (select_hbm, select),
                (column_hbm, column),
                (g1_hbm, g1),
                (g2_hbm, g2),
            )
        )
    ]
    inputs[0].start()
    for at in (5, 2, 3, 4):
        inputs[at].start()
    weights[0].start()

    barrier = pltpu.get_barrier_semaphore()
    for device in list(before.values()) + list(after.values()):
        pl.semaphore_signal(barrier, inc=1, device_id=device, device_id_type=MESH)

    moves = (
        (2, 0, 0, "left"),
        (0, 1, 1, "corner"),
        (4, 0, 1, "left"),
        (6, 1, 0, "left"),
        (1, 1, 2, "up"),
    )
    local = {(0, 2): 3, (0, 3): 5, (1, 3): 7}
    arrivals = {(move[1], move[2]): at for at, move in enumerate(moves)}
    returns = ((6, 0, "left"), (0, 1, "corner"), (1, 2, "up"))

    def remote(source, target, send, recv, device):
        return pltpu.make_async_remote_copy(
            source, target, send, recv, device_id=device, device_id_type=MESH
        )

    labels = [
        remote(region.at[HALF_ROW:], side, esend.at[0], erecv.at[0], before["left"]),
        remote(region.at[:HALF_ROW], corner, esend.at[1], erecv.at[1], before["corner"]),
        remote(region.at[:HALF_ROW], below, esend.at[2], erecv.at[2], before["up"]),
    ]
    forward = [
        remote(own.at[atom], shift.at[window, place], fsend.at[at], frecv.at[at], before[towards])
        for at, (atom, window, place, towards) in enumerate(moves)
    ]
    outward = remote(o_send, o_back, osend.at[0], orecv.at[0], after["left"])

    def first_spot(atom, row):
        return ((atom // 2) * HALF_ROW + row) * columns + (atom % 2) * HALF_COLUMN

    backward = [
        remote(
            ready.at[at, pl.ds(row * HALF_COLUMN, HALF_COLUMN)],
            out_ref.at[pl.ds(first_spot(atom, row), HALF_COLUMN)],
            bsend.at[at * HALF_ROW + row],
            brecv.at[at * HALF_ROW + row],
            after[towards],
        )
        for at, (atom, place, towards) in enumerate(returns)
        for row in range(HALF_ROW)
    ]

    lane = lax.broadcasted_iota(jnp.int32, (1, lanes), 1)
    lane_value = lane.astype(F32)
    low = lane < 64
    scale = 64 ** -0.5
    head_masks = (
        jnp.where(low, scale, 0.0).astype(BF16),
        jnp.where(low, 0.0, scale).astype(BF16),
    )

    def tile(at):
        return slice(at * lanes, (at + 1) * lanes)

    def mark(block, at, places):
        index = 2 * block + at
        count = HALF_ROW * levels
        regions[index] = jnp.zeros(regions.shape[1:], F32)
        for place, (source, row) in enumerate(places):
            for r in range(HALF_ROW):
                start = place * count + r * levels
                regions[index, start : start + levels, :columns] = source[row + r].astype(F32)
        if block == 1:
            wrapped = jnp.where(lat == lat_count - 1, 8.0, 0.0) if at == 1 else 0.0
            regions[index, 4 * count : 4 * count + 1, :] = jnp.where(lane == SPOT, 4.0, 0.0)
            regions[index, 4 * count + 1 : 4 * count + 2, :] = jnp.where(lane == SPOT, wrapped, 0.0)
        value = dot(select[block], regions[index].astype(BF16)) * column[...]
        same = jnp.sum(value, axis=-1, keepdims=True) == lane_value
        marks_q[index] = jnp.where(same, FAR, 0.0).astype(BF16)
        marks_k[index] = jnp.where(same, 0.0, 1.0).astype(BF16)

    def project(block, at, spans, first=False):
        index = 2 * block + at
        rows = jnp.concatenate([xs[index, span_at, :] for span_at in spans], axis=0)
        n1 = normed(rows, g1[block : block + 1, :])
        if first:
            weights[block * 4].wait()
        if first and block == 0:
            inputs[1].start()
            inputs[6].start()
            for later in (1, 2, 3):
                weights[later].start()
        mixed = dot(n1, wqkv[block]).astype(BF16)
        start = 0
        for span_at in spans:
            size = span_at.stop - span_at.start
            qkv[index, span_at, :] = mixed[start : start + size]
            start += size

    whole = (slice(0, span),)
    near = (slice(half, group), slice(group + half, span))
    far = (slice(0, half), slice(group, group + half))

    cut = -(-half // 16) * 16

    def attend(block, at, first=0, last=0):
        index = 2 * block + at
        last = last or group
        size = last - first
        ones = jnp.ones((group, lanes), BF16)
        jobs = [(start, at_tile) for start in (0, group) for at_tile in range(lane_tiles)]
        scored, weighted = {}, {}

        def score(start, at_tile):
            rows = slice(start, start + group)
            asked = slice(start + first, start + last)
            mark_q = marks_q[index, asked, :]
            query = qkv[index, asked, tile(at_tile)]
            query = jnp.concatenate([query * head_masks[0], query * head_masks[1]], axis=0)
            key = qkv[index, rows, tile(lane_tiles + at_tile)]
            return dot_t(
                jnp.concatenate([query, jnp.concatenate([mark_q, mark_q], axis=0)], axis=1),
                jnp.concatenate([key, marks_k[index, rows, :]], axis=1),
            )

        def weigh(scores):
            peak = jnp.max(scores, axis=-1, keepdims=True)
            return jnp.exp(scores - peak).astype(BF16)

        def mix(start, at_tile, weight):
            rows = slice(start, start + group)
            value = qkv[index, rows, tile(2 * lane_tiles + at_tile)]
            total = dot(weight, jnp.concatenate([value, ones], axis=1))
            over = jnp.where(low, total[:size, :lanes], total[size:, :lanes])
            under = jnp.where(low, total[:size, lanes:], total[size:, lanes:])
            asked = slice(start + first, start + last)
            heads[index, asked, tile(at_tile)] = over / under

        for at_job in range(len(jobs) + 2):
            if at_job < len(jobs):
                scored[at_job] = score(*jobs[at_job])
            if 0 <= at_job - 1 < len(jobs):
                weighted[at_job - 1] = weigh(scored.pop(at_job - 1))
            if at_job >= 2:
                mix(*jobs[at_job - 2], weighted.pop(at_job - 2))

    def gather(source, parts):
        pieces = []
        for index, which in parts:
            for start in (which * half, group + which * half):
                pieces.append(source[index, start : start + half, :])
        return jnp.concatenate(pieces, axis=0)

    def mlp(block, h, mixed, first=False):
        if first:
            weights[block * 4 + 1].wait()
        h = h + dot(mixed, wproj[block])
        n2 = normed(h, g2[block : block + 1, :])
        if first:
            weights[block * 4 + 2].wait()
        count = h.shape[0]
        for at in range(0, hidden, step):
            inner[:count, at : at + step] = gelu(
                dot(n2, wup[block, :, at : at + step]).astype(BF16)
            )
        if first:
            weights[block * 4 + 3].wait()
        return h + dot(inner[:count, :], wdown[block])

    def relevel(slot, h, shifts, targets, stride):
        for at in range(lane_tiles):
            flat[slot, at] = h[:, tile(at)]
        for place, target in enumerate(targets):
            for at in range(lane_tiles):
                for group_at in range(2):
                    for lev in range(WLEV):
                        source = group_at * half + place * QUARTER + lev
                        target[at, pl.ds(shifts[group_at][lev], CELL, stride=stride)] = flat[
                            slot, at, pl.ds(source, CELL, stride=WLEV)
                        ]

    def finish_first(slot, h, atoms):
        targets = [cross.at[slot, place] for place in range(2)]
        relevel(slot, h, ((QUARTER + 1, 0), (1, QUARTER)), targets, WLEV)
        for place, atom in enumerate(atoms):
            for at in range(lane_tiles):
                own[atom, :, tile(at)] = cross[slot, place, at].astype(BF16)

    def finish_second(slot, h, results):
        targets = [wide.at[slot, place] for place in range(2)]
        relevel(slot, h, ((1, 2), (3, 0)), targets, levels)
        for place, result in enumerate(results):
            for spot in range(CELL):
                row, col = divmod(spot, HALF_COLUMN)
                for at in range(lane_tiles):
                    value = wide[slot, place, at, spot * levels : (spot + 1) * levels].astype(BF16)
                    if result[0] == "out":
                        out_ref[first_spot(result[1], row) + col, at] = value
                    else:
                        ready[result[1], spot, at] = value
            if result[0] == "send":
                for row in range(HALF_ROW):
                    backward[result[1] * HALF_ROW + row].start()

    def load_first(u):
        if u:
            inputs[u].wait()
        for spot in range(window_spots):
            row, col = divmod(spot, columns)
            place = (col // HALF_COLUMN) * 2 + row // HALF_ROW
            at_spot = (row % HALF_ROW) * HALF_COLUMN + col % HALF_COLUMN
            start = place * QUARTER + at_spot * WLEV
            for at in range(lane_tiles):
                value = xin[u * window_spots + spot, at].astype(F32)
                for group_at in range(2):
                    xs[u, group_at * group + start : group_at * group + start + WLEV, tile(at)] = (
                        value[group_at * WLEV : (group_at + 1) * WLEV]
                    )

    def own_regions(u):
        places = [(region, u * WLAT), (region, u * WLAT + HALF_ROW)]
        return places + places

    def load_second(w, places):
        for place in places:
            if (w, place) in arrivals:
                forward[arrivals[w, place]].wait_recv()
                value = shift[w, place].astype(F32)
            else:
                value = own[local[w, place]].astype(F32)
            for group_at in range(2):
                start = group_at * group + place * QUARTER
                xs[2 + w, start : start + QUARTER, :] = value[
                    group_at * QUARTER : (group_at + 1) * QUARTER
                ]

    inputs[0].wait()
    load_first(0)
    inputs[2].wait()
    inputs[3].wait()
    inputs[4].wait()
    mark(0, 0, own_regions(0))
    inputs[5].wait()
    project(0, 0, whole, True)
    pl.semaphore_wait(barrier, 6)
    for copy in labels:
        copy.start()
    attend(0, 0, 0, cut)
    inputs[6].wait()
    h = mlp(0, gather(xs, [(0, 0)]), gather(heads, [(0, 0)]).astype(BF16), True)
    finish_first(0, h, (0, 2))
    forward[0].start()
    forward[1].start()
    for at in range(4, 8):
        weights[at].start()
    load_first(1)
    mark(0, 1, own_regions(1))
    project(0, 1, whole)
    attend(0, 1, 0, cut)
    h = mlp(0, gather(xs, [(1, 0)]), gather(heads, [(1, 0)]).astype(BF16))
    finish_first(1, h, (4, 6))
    forward[2].start()
    forward[3].start()
    attend(0, 0, cut, group)
    attend(0, 1, cut, group)
    parts = [(0, 1), (1, 1)]
    h = mlp(0, gather(xs, parts), gather(heads, parts).astype(BF16))
    finish_first(0, h[:group], (1, 3))
    forward[4].start()
    finish_first(1, h[group:], (5, 7))

    for copy in labels:
        copy.wait_recv()
    load_second(0, (2, 3))
    project(1, 0, near, True)
    mark(1, 0, [(side, 0), (side, HALF_ROW), (region, HALF_ROW), (region, 2 * HALF_ROW)])
    mark(1, 1, [(side, 2 * HALF_ROW), (corner, 0), (below, 0), (region, 3 * HALF_ROW)])
    load_second(0, (0, 1))
    project(1, 0, far)
    attend(1, 0)
    o_send[...] = gather(heads, [(2, 0)]).astype(BF16)
    outward.start()
    load_second(1, (0, 1, 2, 3))
    project(1, 1, whole)
    attend(1, 1)
    h = mlp(1, gather(xs, [(3, 0)]), gather(heads, [(3, 0)]).astype(BF16), True)
    finish_second(0, h, (("send", 0), ("send", 1)))
    parts = [(3, 1), (2, 1)]
    h = mlp(1, gather(xs, parts), gather(heads, parts).astype(BF16))
    finish_second(1, h[:group], (("send", 2), ("out", 7)))
    finish_second(0, h[group:], (("out", 3), ("out", 5)))
    pieces = [own[2].astype(F32), own[4].astype(F32)]
    residual = jnp.concatenate(
        [piece[:QUARTER] for piece in pieces] + [piece[QUARTER:] for piece in pieces], axis=0
    )
    outward.wait_recv()
    h = mlp(1, residual, o_back[...])
    finish_second(1, h, (("out", 2), ("out", 4)))
    for copy in backward:
        copy.wait_recv()
    for copy in labels + forward + [outward] + backward:
        copy.wait_send()


def settle(source, target, sems):
    chunks = sems.shape[0]
    size = source.shape[0] // chunks
    copies = [
        pltpu.make_async_copy(
            source.at[pl.ds(at * size, size)], target.at[pl.ds(at * size, size)], sems.at[at]
        )
        for at in range(chunks)
    ]
    for copy in copies:
        copy.start()
    for copy in copies:
        copy.wait()


def per_device(
    tokens, region, norm_gain1, qkv_weight, proj_weight, norm_gain2, up_weight, down_weight
):
    levels, row_count, column_count, features = tokens.shape
    hidden = up_weight.shape[2]
    lane_tiles = features // LANES
    spots = row_count * column_count
    quarter_rows = levels * CELL
    span = 4 * quarter_rows
    group = span // 2
    x = jnp.transpose(tokens.reshape(levels, spots, lane_tiles, LANES), (1, 2, 0, 3))
    marks = jnp.transpose(region, (1, 0, 2))
    select, column = label_tables(levels)

    vmem = pl.BlockSpec(memory_space=pltpu.VMEM)
    hbm = pl.BlockSpec(memory_space=pl.ANY)
    dma = pltpu.SemaphoreType.DMA
    out = pl.pallas_call(
        kernel,
        out_shape=pltpu.VMEM(x.shape, BF16),
        in_specs=[hbm] * 10,
        out_specs=vmem,
        scratch_shapes=[
            pltpu.VMEM(x.shape, BF16),
            pltpu.VMEM(marks.shape, jnp.int32),
            pltpu.VMEM(select.shape, BF16),
            pltpu.VMEM(column.shape, F32),
            pltpu.VMEM(norm_gain1.shape, F32),
            pltpu.VMEM(norm_gain2.shape, F32),
            pltpu.VMEM((4, LANES, LANES), F32),
            pltpu.VMEM((8, quarter_rows, features), BF16),
            pltpu.VMEM((2, 4, quarter_rows, features), BF16),
            pltpu.VMEM((row_count - HALF_ROW,) + marks.shape[1:], jnp.int32),
            pltpu.VMEM((HALF_ROW,) + marks.shape[1:], jnp.int32),
            pltpu.VMEM((HALF_ROW,) + marks.shape[1:], jnp.int32),
            pltpu.VMEM((4, span, features), F32),
            pltpu.VMEM((4, span, 3 * features), BF16),
            pltpu.VMEM((4, span, features), F32),
            pltpu.VMEM((4, span, LANES), BF16),
            pltpu.VMEM((4, span, LANES), BF16),
            pltpu.VMEM((span, hidden), BF16),
            pltpu.VMEM((2, lane_tiles, group, LANES), F32),
            pltpu.VMEM((2, 2, lane_tiles, quarter_rows, LANES), F32),
            pltpu.VMEM((2, 2, lane_tiles, quarter_rows, LANES), F32),
            pltpu.VMEM((3, CELL) + x.shape[1:], BF16),
            pltpu.VMEM((group, features), BF16),
            pltpu.VMEM((group, features), BF16),
            pltpu.VMEM(qkv_weight.shape, BF16),
            pltpu.VMEM(proj_weight.shape, BF16),
            pltpu.VMEM(up_weight.shape, BF16),
            pltpu.VMEM(down_weight.shape, BF16),
            dma((8,)),
            dma((7,)),
            dma((5,)),
            dma((5,)),
            dma((3,)),
            dma((3,)),
            dma((1,)),
            dma((1,)),
            dma((3 * HALF_ROW,)),
            dma((3 * HALF_ROW,)),
        ],
        compiler_params=pltpu.CompilerParams(
            collective_id=0, has_side_effects=True, vmem_limit_bytes=54 * 1024 * 1024
        ),
    )(
        x, marks, select, column, norm_gain1, norm_gain2,
        qkv_weight, proj_weight, up_weight, down_weight,
    )
    out = pl.pallas_call(
        settle,
        out_shape=jax.ShapeDtypeStruct(x.shape, BF16),
        in_specs=[vmem],
        out_specs=hbm,
        scratch_shapes=[dma((8,))],
        compiler_params=pltpu.CompilerParams(vmem_limit_bytes=2 * 1024 * 1024),
    )(out)
    return jnp.transpose(out, (2, 0, 1, 3)).reshape(tokens.shape)


def solution(mesh):
    return jax.shard_map(
        per_device,
        mesh=mesh,
        in_specs=(P(None, "lat", "lon", None), P(None, "lat", "lon"), P(), P(), P(), P(), P(), P()),
        out_specs=P(None, "lat", "lon", None),
        check_vma=False,
    )
```
